32 devices in a mesh: rep: 2 (over x), shard: 16 (over z, y, core).
Axes of the slice: x: 2, y: 2, z: 4, core: 2. Of those that a mesh axis runs over, the one named last changes fastest.
Arguments:
- tokens_x: bfloat16 [8192, 4096], P(('rep', 'shard')), may hold values from -6 to 6
- key_grad: bfloat16 [8192, 1024], P(('rep', 'shard')), may hold values from -0.06591797 to 0.06591797
- left_root: bfloat16 [64, 512, 512], P('shard'), may hold values from -1 to 3
- slot_grads: bfloat16 [64, 512, 512], P('shard'), may hold values from -6 to 6
- right_root: bfloat16 [64, 512, 512], P('shard'), may hold values from -1 to 3
- block_slot: int32 [32], replicated, may hold values from 0 to 63, as said below
Outputs:
- grad_key: float32 [4096, 1024], P('shard')
- update: bfloat16 [512, 32, 512], P('shard')
The draws below stay inside these ranges and needn't reach their ends.
Inputs may be any that keep to these rules, and one draw needn't show every extreme that they name: `block_slot`: the entries are distinct; slot v is slot v % 4 of shard index v // 4; no shard index holds more than 4 blocks, and some shard index holds exactly 4.
All inputs are finite; a program needn't handle non-finite values.
Results may differ from the reference program's by a relative error of at most 0.006.
Values may be sent and summed in bfloat16 or wider, within the bound.
A program may use at most 128 MiB of HBM per device.

```python
import jax
import jax.numpy as jnp
from jax import lax

D = 4096
KEY_WIDTH = 1024
TOK_DEV = 256
BLOCK = 512
SLOTS = 4
NBLK = 32
SLOT_ALL = 64
TOKENS = 8192


def root_matrix(key):
    first_key, second_key = jax.random.split(key)
    diagonal = jnp.exp(jax.random.uniform(first_key, (SLOT_ALL, BLOCK), jnp.float32, jnp.log(0.5), jnp.log(2.0)))
    noise = jax.random.normal(second_key, (SLOT_ALL, BLOCK, BLOCK), jnp.float32)
    symmetric = (noise + jnp.swapaxes(noise, 1, 2)) * (0.5 / (2.0 * BLOCK) ** 0.5)
    symmetric = jnp.clip(symmetric, -0.9, 0.9)
    identity = jnp.eye(BLOCK, dtype=jnp.float32)
    return (symmetric + diagonal[:, :, None] * identity[None, :, :]).astype(jnp.bfloat16)


def draw_left_root(key, part):
    return root_matrix(jax.random.fold_in(key, 11))


def draw_right_root(key, part):
    return root_matrix(jax.random.fold_in(key, 23))


def draw_block_slot(key, part):
    base_key = jax.random.fold_in(key, 37)
    first_key, second_key, third_key = jax.random.split(base_key, 3)
    full_owner = jax.random.randint(first_key, (), 0, SLOT_ALL // SLOTS)
    slot_ids = jnp.arange(SLOT_ALL, dtype=jnp.int32)
    ranking = jax.random.permutation(second_key, SLOT_ALL).astype(jnp.int32)
    ranking = jnp.where(slot_ids // SLOTS == full_owner, slot_ids % SLOTS - SLOTS, ranking)
    chosen = jnp.argsort(ranking, stable=True)[:NBLK].astype(jnp.int32)
    shuffled = jax.random.permutation(third_key, NBLK).astype(jnp.int32)
    return chosen[shuffled].astype(jnp.int32)


def strengthened(array, rng, source, target, parts, factor):
    def block_of(position):
        return (jnp.arange(array.shape[position]) // (array.shape[position] // parts)).reshape((-1,) + (1,) * (array.ndim - 1 - position))

    near = jax.random.permutation(rng, parts)[block_of(target)]
    second = (block_of(target) + parts // 2) % parts
    return jnp.where((block_of(source) == near) | (block_of(source) == second), factor * array, array)


def block_levels(own_key, shape, cuts, least, top_value):
    gain, own = 1.0, jax.random.fold_in(own_key, 6)
    for axis_at, shards_of in cuts:
        draws = jnp.exp(jax.random.uniform(jax.random.fold_in(own, axis_at), (shards_of,), jnp.float32, least / len(cuts), top_value / len(cuts)))
        gain = gain * jnp.repeat(draws, shape[axis_at] // shards_of).reshape([-1 if axis == axis_at else 1 for axis in range(len(shape))])
    return gain


def normal_values(rng, dims, scale, reach, cuts=(), kind=jnp.bfloat16):
    entries = jax.random.normal(rng, dims, jnp.float32) * scale
    if len(cuts) > 0:
        entries = block_levels(rng, dims, cuts, -0.22, 0.18) * entries
    return jnp.clip(entries, min=-reach, max=reach).astype(kind)


def noise_with(stream_key, extent, spread, reach, cuts, heavy, kind=jnp.bfloat16):
    drawn = spread * jax.random.normal(stream_key, extent, jnp.float32)
    if cuts:
        drawn = drawn * block_levels(stream_key, extent, cuts, -0.22, 0.18)
    return jnp.clip(strengthened(drawn, jax.random.fold_in(stream_key, 3), *heavy), -reach, reach).astype(kind)


def setup_inputs(seed: int = 0) -> dict:
    keys = jax.random.split(jax.random.key(seed), 7)
    return {
        "tokens_x": noise_with(keys[0], (TOKENS, D), 1.0, 6.0, ((0, 32),), (0, 1, 32, 2.75)),
        "key_grad": normal_values(keys[1], (TOKENS, KEY_WIDTH), (TOKENS ** -0.5), 0.06591797, ((0, 32),)),
        "left_root": draw_left_root(jax.random.fold_in(keys[6], 71), 0),
        "slot_grads": normal_values(keys[3], (SLOT_ALL, BLOCK, BLOCK), 1.0, 6.0, ((0, 16),)),
        "right_root": draw_right_root(jax.random.fold_in(keys[6], 71), 0),
        "block_slot": draw_block_slot(jax.random.fold_in(keys[6], 71), 0),
    }


def reference(tokens_x, key_grad, left_root, slot_grads, right_root, block_slot):
    step_count = TOKENS // TOK_DEV
    token_blocks = tokens_x.reshape(step_count, TOK_DEV, D)
    grad_blocks = key_grad.reshape(step_count, TOK_DEV, KEY_WIDTH)

    def accumulate(total, pieces):
        rows_in, grads_in = pieces
        added = jnp.dot(rows_in.astype(jnp.float32).T, grads_in.astype(jnp.float32), preferred_element_type=jnp.float32)
        return total + added, None

    grad_key, ignored = lax.scan(accumulate, jnp.zeros((D, KEY_WIDTH), jnp.float32), (token_blocks, grad_blocks))

    def precondition(slot_index):
        left_part = jnp.dot(left_root[slot_index].astype(jnp.float32), slot_grads[slot_index].astype(jnp.float32), preferred_element_type=jnp.float32).astype(jnp.bfloat16)
        return jnp.dot(left_part.astype(jnp.float32), right_root[slot_index].astype(jnp.float32), preferred_element_type=jnp.float32).astype(jnp.bfloat16)

    blocks = lax.map(precondition, block_slot)
    update = jnp.transpose(blocks, (1, 0, 2))
    return grad_key, update
```

```python
import jax
import jax.numpy as jnp
from jax import lax
from jax.experimental import pallas as pl
from jax.experimental.pallas import tpu as pltpu
from jax.sharding import PartitionSpec as P

MESH = pl.DeviceIdType.MESH
GROUP = 4
PARTS = 2
PIECES = 2


def column_term(features, cotangent):
    return lax.dot_general(
        features, cotangent, (((0,), (0,)), ((), ())), preferred_element_type=jnp.float32
    )


def precondition(left_block, grad_block, right_block):
    left_part = jnp.einsum(
        "sij,sjk->sik", left_block, grad_block, preferred_element_type=jnp.float32
    ).astype(jnp.bfloat16)
    return jnp.einsum(
        "sij,sjk->isk", left_part, right_block, preferred_element_type=jnp.float32
    ).astype(jnp.bfloat16)


def plain_shards(tokens_x, key_grad, left_root, slot_grads, right_root, block_slot):
    n_shard = lax.axis_size("shard")
    n_rep = lax.axis_size("rep")
    own_rows = lax.psum_scatter(
        column_term(tokens_x, key_grad), "shard", scatter_dimension=0, tiled=True
    )
    grad_key = lax.psum(own_rows, "rep")
    slot_count = left_root.shape[0]
    half_slots = slot_count // n_rep
    first_slot = lax.axis_index("rep") * half_slots

    def own_half(values):
        return lax.dynamic_slice_in_dim(values, first_slot, half_slots, 0)

    product = precondition(own_half(left_root), own_half(slot_grads), own_half(right_root))
    received = lax.all_to_all(product, "shard", split_axis=0, concat_axis=1, tiled=True)
    joined = lax.all_gather(received, "rep", axis=1, tiled=True)
    owner = block_slot // slot_count
    within = block_slot % slot_count
    position = (
        within // half_slots * (n_shard * half_slots) + owner * half_slots + within % half_slots
    )
    update = jnp.take(joined, position, axis=1)
    return (grad_key, update)


def remote(src, dst, send_sem, recv_sem, target):
    return pltpu.make_async_remote_copy(
        src_ref=src,
        dst_ref=dst,
        send_sem=send_sem,
        recv_sem=recv_sem,
        device_id=target,
        device_id_type=MESH,
    )


def kernel(
    slot_ref, x_ref, g_ref, lr_ref, sg_ref, rr_ref, og_ref, ou_ref,
    x_all, g_all, lr, sg, rr, prod, relay, upd, hot, part, met, kept, passed, first, second,
    sums, rows,
    load_sem, x_load, out_sem, send_sem, g_recv, x_recv, u_recv, y_recv, a_recv, s_recv, t_recv,
    r_recv, v_recv,
):
    me = lax.axis_index("shard")
    rep = lax.axis_index("rep")
    other_rep = 1 - rep
    q = me % GROUP
    z = me // GROUP
    base = z * GROUP
    core = q + 1 - 2 * (q % 2)
    far = (q + 2) % GROUP
    both = (core + 2) % GROUP
    relatives = (q, core, far, both)
    z_near = z + 1 - 2 * (z % 2)
    z_half = (z + 2) % 4
    z_last = 3 - z
    order_of = (z_last, z_near, z_half, z)
    tok = g_ref.shape[0]
    unit = met.shape[1]
    half = met.shape[2]
    slots = lr.shape[0]
    n = lr.shape[1]
    height = lr.shape[2]
    width = lr.shape[3]
    blocks = slot_ref.shape[0]
    piece = width // PIECES

    def shard(index):
        return {"shard": index}

    across = {"rep": other_rep}
    near = shard(z_near * GROUP + q)
    opposite = shard(z_half * GROUP + q)

    def tokens_of(index):
        return pl.ds(index * tok, tok)

    def keys_of(side):
        return pl.ds(pl.multiple_of(side * half, 128), half)

    def columns(o, index, r):
        start = (order_of[o] * GROUP + index) * (PARTS * unit) + r * unit
        return pl.ds(pl.multiple_of(start, 128), unit)

    def unit_of(r):
        return pl.ds(r * unit, unit)

    copy_lr = pltpu.make_async_copy(lr_ref.at[:, :, rep], lr, load_sem.at[0])
    copy_sg = pltpu.make_async_copy(sg_ref, sg, load_sem.at[1])
    copy_rr = pltpu.make_async_copy(rr_ref, rr, load_sem.at[2])
    copy_g = pltpu.make_async_copy(g_ref, g_all.at[tokens_of(q)], load_sem.at[3])
    copies_x = []
    for o in range(4):
        start = pl.multiple_of((order_of[o] * GROUP + q) * (PARTS * unit), 128)
        copies_x.append(
            pltpu.make_async_copy(
                x_ref.at[:, pl.ds(start, PARTS * unit)], x_all.at[o, tokens_of(q)], x_load.at[o]
            )
        )

    barrier = pltpu.get_barrier_semaphore()
    peers = [across]
    for index in (core, far, both):
        peers.append(shard(base + index))
    for level in (z_near, z_half, z_last):
        peers.append(shard(level * GROUP + q))
    for peer in peers:
        pl.semaphore_signal(barrier, inc=1, device_id=peer, device_id_type=MESH)
    copy_lr.start()
    copy_sg.start()
    copy_rr.start()
    copy_g.start()
    for copy in copies_x:
        copy.start()
    pl.semaphore_wait(barrier, len(peers))

    def send(src, dst, kind, recv_sem, target):
        remote(src, dst, send_sem.at[kind], recv_sem, target).start()

    def arrive(ref, recv_sem):
        remote(ref, ref, send_sem.at[0], recv_sem, across).wait_recv()

    def send_g(which, target, place):
        keys = keys_of(other_rep if which == 0 else rep)
        send(
            g_ref.at[:, keys], g_all.at[tokens_of(q), keys], 0, g_recv.at[which, place],
            shard(base + target),
        )

    def send_x(o, r):
        for target in (far, both, core):
            send(
                x_ref.at[:, columns(o, target, r)],
                x_all.at[o, tokens_of(q), unit_of(r)],
                1,
                x_recv.at[o, r],
                shard(base + target),
            )

    send_g(0, far, 0)
    send_g(0, core, 1)
    for r in range(PARTS):
        send_x(0, r)
    for r in range(PARTS):
        send_x(1, r)
    send_g(1, far, 0)
    send_g(1, core, 1)
    for o in (2, 3):
        for r in range(PARTS):
            send_x(o, r)

    chosen = jnp.zeros((blocks, 128), jnp.int32)
    row = lax.broadcasted_iota(jnp.int32, (blocks, 128), 0)
    for b in range(blocks):
        chosen = jnp.where(row == b, slot_ref[b], chosen)
    lane = lax.broadcasted_iota(jnp.int32, (blocks, 128), 1)
    per = 4 * slots * height
    for k, index in enumerate(relatives):
        for part_of in range(per // 128):
            place = lane + part_of * 128
            source = place // (slots * height) * (GROUP * slots) + index * slots
            source = source + place // height % slots
            same = source == chosen
            for i in range(height):
                hit = jnp.logical_and(same, place % height == i)
                hot[k, pl.ds(i * blocks, blocks), pl.ds(part_of * 128, 128)] = jnp.where(
                    hit, 1.0, 0.0
                ).astype(jnp.bfloat16)

    copy_lr.wait()
    copy_sg.wait()
    copy_rr.wait()
    for s in range(slots):
        left = jnp.dot(
            lr[s].reshape(n * height, width), sg[s], preferred_element_type=jnp.float32
        ).astype(jnp.bfloat16)
        full = jnp.dot(left, rr[s], preferred_element_type=jnp.float32).astype(jnp.bfloat16)
        prod[:, s] = full.reshape(4, GROUP, height, width)
    for level in (z_half, z_last, z_near):
        send(prod.at[level], relay.at[z], 2, u_recv.at[0], shard(level * GROUP + q))
    relay[z] = prod[z]

    def gather_g(which):
        keys = keys_of(other_rep if which == 0 else rep)
        view = g_all.at[tokens_of(far), keys]
        arrive(view, g_recv.at[which, 0])
        send(view, view, 0, g_recv.at[which, 2], shard(base + core))
        arrive(g_all.at[tokens_of(core), keys], g_recv.at[which, 1])
        arrive(g_all.at[tokens_of(both), keys], g_recv.at[which, 2])

    def partial(o, r, side):
        return lax.dot_general(
            x_all[o, :, r * unit : (r + 1) * unit],
            g_all[:, keys_of(side)],
            (((0,), (0,)), ((), ())),
            preferred_element_type=jnp.float32,
        )

    def give(o, r):
        if r == 0:
            copies_x[o].wait()
        arrive(x_all.at[o, pl.ds(0, 3 * tok), unit_of(r)], x_recv.at[o, r])
        part[o * PARTS + r] = partial(o, r, other_rep).astype(jnp.bfloat16)
        send(
            part.at[o * PARTS + r], met.at[o * PARTS + r], 3, a_recv.at[o * PARTS + r], across
        )

    def keep(o, r):
        kept[o * PARTS + r] = partial(o, r, rep)

    def total_of(o, r):
        u = o * PARTS + r
        arrive(met.at[u], a_recv.at[u])
        return kept[u] + met[u].astype(jnp.float32)

    def pass_near(o, r):
        u = o * PARTS + r
        passed[u] = total_of(o, r).astype(jnp.bfloat16)
        send(passed.at[u], first.at[u], 4, s_recv.at[u], near)

    def pass_half(r):
        u = 2 * PARTS + r
        total = total_of(2, r)
        arrive(first.at[r], s_recv.at[r])
        passed[u] = (total + first[r].astype(jnp.float32)).astype(jnp.bfloat16)
        send(passed.at[u], second.at[r], 5, t_recv.at[r], opposite)

    def finish(r):
        total = total_of(3, r)
        arrive(first.at[PARTS + r], s_recv.at[PARTS + r])
        total = total + first[PARTS + r].astype(jnp.float32)
        arrive(second.at[r], t_recv.at[r])
        total = total + second[r].astype(jnp.float32)
        view = sums.at[rep, unit_of(r)]
        sums[rep, unit_of(r)] = total.astype(jnp.bfloat16)
        send(view, view, 6, r_recv.at[r], across)

    def slice_of(p):
        return pl.ds(p * piece, piece)

    def spread():
        arrive(relay.at[pl.ds(0, 3)], u_recv.at[0])
        for p in range(PIECES):
            for k, target in ((2, far), (3, both), (1, core)):
                send(
                    relay.at[:, :, target, :, slice_of(p)],
                    upd.at[k, :, :, :, slice_of(p)],
                    7,
                    y_recv.at[p],
                    shard(base + target),
                )

    def select(p):
        cols = slice(p * piece, (p + 1) * piece)
        arrive(upd.at[pl.ds(1, 3), :, :, :, slice_of(p)], y_recv.at[p])
        value = jnp.dot(
            hot[0], relay[:, :, q, :, cols].reshape(per, piece), preferred_element_type=jnp.float32
        )
        for k in range(1, 4):
            value = value + jnp.dot(
                hot[k], upd[k, :, :, :, cols].reshape(per, piece),
                preferred_element_type=jnp.float32,
            )
        rows[rep, :, :, cols] = value.astype(jnp.bfloat16).reshape(height, blocks, piece)
        view = rows.at[rep, :, :, slice_of(p)]
        send(view, view, 8, v_recv.at[p], across)

    copy_g.wait()
    gather_g(0)
    for o in (0, 1):
        for r in range(PARTS):
            give(o, r)
    gather_g(1)
    for o in (0, 1):
        for r in range(PARTS):
            keep(o, r)
            pass_near(o, r)
    give(2, 0)
    keep(2, 0)
    give(2, 1)
    keep(2, 1)
    spread()
    give(3, 0)
    keep(3, 0)
    pass_half(0)
    give(3, 1)
    keep(3, 1)
    pass_half(1)
    for r in range(PARTS):
        finish(r)
    for p in range(PIECES):
        select(p)

    outs = []

    def put(src, dst):
        copy = pltpu.make_async_copy(src, dst, out_sem.at[len(outs)])
        copy.start()
        outs.append(copy)

    put(sums.at[rep], og_ref.at[:, keys_of(rep)])
    put(rows.at[rep], ou_ref.at[rep])
    for r in range(PARTS):
        view = sums.at[other_rep, unit_of(r)]
        arrive(view, r_recv.at[r])
        put(view, og_ref.at[unit_of(r), keys_of(other_rep)])
    for p in range(PIECES):
        view = rows.at[other_rep, :, :, slice_of(p)]
        arrive(view, v_recv.at[p])
        put(view, ou_ref.at[other_rep, :, :, slice_of(p)])

    def drain(ref, kind):
        remote(ref, ref, send_sem.at[kind], send_sem.at[kind], across).wait_send()

    drain(x_all.at[pl.ds(0, 3)], 0)
    drain(x_all.at[pl.ds(0, 3)], 1)
    drain(relay.at[pl.ds(0, 3)], 2)
    drain(met, 3)
    drain(met.at[pl.ds(0, 2 * PARTS)], 4)
    drain(met.at[pl.ds(0, PARTS)], 5)
    drain(met.at[pl.ds(0, PARTS)], 6)
    drain(relay.at[pl.ds(0, 3)], 7)
    drain(rows.at[0], 8)
    for copy in outs:
        copy.wait()


def fused_shards(tokens_x, key_grad, left_root, slot_grads, right_root, block_slot):
    n = lax.axis_size("shard")
    n_rep = lax.axis_size("rep")
    tok, d_model = tokens_x.shape
    key_width = key_grad.shape[1]
    cols = d_model // n
    slots, order_b, width = left_root.shape
    height = order_b // n // n_rep
    blocks = block_slot.shape[0]
    half = key_width // n_rep
    unit = cols // PARTS
    per = 4 * slots * height
    bf16, f32 = jnp.bfloat16, jnp.float32
    dma = pltpu.SemaphoreType.DMA
    any_spec = pl.BlockSpec(memory_space=pl.ANY)
    sums, rows = pl.pallas_call(
        kernel,
        out_shape=(
            jax.ShapeDtypeStruct((cols, key_width), bf16),
            jax.ShapeDtypeStruct((n_rep, height, blocks, width), bf16),
        ),
        in_specs=[pl.BlockSpec(memory_space=pltpu.SMEM)] + [any_spec] * 5,
        out_specs=(any_spec, any_spec),
        scratch_shapes=[
            pltpu.VMEM((4, GROUP * tok, cols), bf16),
            pltpu.VMEM((GROUP * tok, key_width), bf16),
            pltpu.VMEM((slots, n, height, width), bf16),
            pltpu.VMEM(slot_grads.shape, bf16),
            pltpu.VMEM(right_root.shape, bf16),
            pltpu.VMEM((4, slots, GROUP, height, width), bf16),
            pltpu.VMEM((4, slots, GROUP, height, width), bf16),
            pltpu.VMEM((4, 4, slots, height, width), bf16),
            pltpu.VMEM((4, height * blocks, per), bf16),
            pltpu.VMEM((4 * PARTS, unit, half), bf16),
            pltpu.VMEM((4 * PARTS, unit, half), bf16),
            pltpu.VMEM((4 * PARTS, unit, half), f32),
            pltpu.VMEM((3 * PARTS, unit, half), bf16),
            pltpu.VMEM((2 * PARTS, unit, half), bf16),
            pltpu.VMEM((PARTS, unit, half), bf16),
            pltpu.VMEM((n_rep, cols, half), bf16),
            pltpu.VMEM((n_rep, height, blocks, width), bf16),
            dma((4,)),
            dma((4,)),
            dma((2 + PARTS + PIECES,)),
            dma((9,)),
            dma((2, 3)),
            dma((4, PARTS)),
            dma((1,)),
            dma((PIECES,)),
            dma((4 * PARTS,)),
            dma((2 * PARTS,)),
            dma((PARTS,)),
            dma((PARTS,)),
            dma((PIECES,)),
        ],
        compiler_params=pltpu.CompilerParams(
            collective_id=0, has_side_effects=True, vmem_limit_bytes=60 * 1024 * 1024
        ),
    )(
        block_slot,
        tokens_x,
        key_grad,
        left_root.reshape(slots, n, n_rep, height, width),
        slot_grads,
        right_root,
    )
    return (sums.astype(f32), rows.reshape(n_rep * height, blocks, width))


def shards(tokens_x, key_grad, left_root, slot_grads, right_root, block_slot):
    n = lax.axis_size("shard")
    n_rep = lax.axis_size("rep")
    cols = tokens_x.shape[1] // n
    width = left_root.shape[2]
    per = left_root.shape[0] * left_root.shape[1] // (GROUP * n_rep)
    aligned = (
        n_rep == 2
        and n == 4 * GROUP
        and tokens_x.shape[1] % (n * PARTS * 128) == 0
        and key_grad.shape[1] % (n_rep * 128) == 0
        and 2 * key_grad.shape[1] == GROUP * PARTS * cols
        and tokens_x.shape[0] % 16 == 0
        and left_root.shape[1] % (n * n_rep * 16) == 0
        and width % (PIECES * 128) == 0
        and per % 128 == 0
        and block_slot.shape[0] % 16 == 0
    )
    program = fused_shards if aligned else plain_shards
    return program(tokens_x, key_grad, left_root, slot_grads, right_root, block_slot)


def solution(mesh):
    return jax.shard_map(
        shards,
        mesh=mesh,
        in_specs=(
            P(("rep", "shard"), None),
            P(("rep", "shard"), None),
            P("shard", None, None),
            P("shard", None, None),
            P("shard", None, None),
            P(),
        ),
        out_specs=(P("shard", None), P("shard", None, None)),
        check_vma=False,
    )
```

```python
import jax
import jax.numpy as jnp
from jax import lax
from jax.experimental import pallas as pl
from jax.experimental.pallas import tpu as pltpu
from jax.sharding import PartitionSpec as P

MESH = pl.DeviceIdType.MESH
GROUP = 4
PARTS = 2
PIECES = 4


def column_term(features, cotangent):
    return lax.dot_general(
        features, cotangent, (((0,), (0,)), ((), ())), preferred_element_type=jnp.float32
    )


def precondition(left_block, grad_block, right_block):
    left_part = jnp.einsum(
        "sij,sjk->sik", left_block, grad_block, preferred_element_type=jnp.float32
    ).astype(jnp.bfloat16)
    return jnp.einsum(
        "sij,sjk->isk", left_part, right_block, preferred_element_type=jnp.float32
    ).astype(jnp.bfloat16)


def plain_shards(tokens_x, key_grad, left_root, slot_grads, right_root, block_slot):
    n_shard = lax.axis_size("shard")
    n_rep = lax.axis_size("rep")
    own_rows = lax.psum_scatter(
        column_term(tokens_x, key_grad), "shard", scatter_dimension=0, tiled=True
    )
    grad_key = lax.psum(own_rows, "rep")
    slot_count = left_root.shape[0]
    half_slots = slot_count // n_rep
    first_slot = lax.axis_index("rep") * half_slots

    def own_half(values):
        return lax.dynamic_slice_in_dim(values, first_slot, half_slots, 0)

    product = precondition(own_half(left_root), own_half(slot_grads), own_half(right_root))
    received = lax.all_to_all(product, "shard", split_axis=0, concat_axis=1, tiled=True)
    joined = lax.all_gather(received, "rep", axis=1, tiled=True)
    owner = block_slot // slot_count
    within = block_slot % slot_count
    position = (
        within // half_slots * (n_shard * half_slots) + owner * half_slots + within % half_slots
    )
    update = jnp.take(joined, position, axis=1)
    return (grad_key, update)


def remote(src, dst, send_sem, recv_sem, target):
    return pltpu.make_async_remote_copy(
        src_ref=src,
        dst_ref=dst,
        send_sem=send_sem,
        recv_sem=recv_sem,
        device_id=target,
        device_id_type=MESH,
    )


def kernel(
    slot_ref, x_ref, g_ref, lr_ref, sg_ref, rr_ref, og_ref, ou_ref,
    x_all, g_all, lr, sg, rr, prod, relay, upd, hot, part, met, kept, passed, first, second,
    x_own, part_own, met_own, kept_own, turned, got,
    sums, rows, wide,
    open_sem, load_sem, x_load, out_sem, send_sem, g_recv, x_recv, u_recv, y_recv, a_recv, s_recv, t_recv,
    r_recv, v_recv, d_load, d_recv, e_recv, f_recv,
):
    me = lax.axis_index("shard")
    rep = lax.axis_index("rep")
    other_rep = 1 - rep
    q = me % GROUP
    z = me // GROUP
    base = z * GROUP
    core = q + 1 - 2 * (q % 2)
    far = (q + 2) % GROUP
    both = (core + 2) % GROUP
    relatives = (q, core, far, both)
    z_near = z + 1 - 2 * (z % 2)
    z_half = (z + 2) % 4
    z_last = 3 - z
    order_of = (z_last, z_half, z_near, z)
    tok = g_ref.shape[0]
    unit = met.shape[1]
    half = met.shape[2]
    slots = lr.shape[0]
    n = lr.shape[1]
    height = lr.shape[2]
    width = lr.shape[3]
    blocks = slot_ref.shape[0]
    piece = width // PIECES

    def shard(index):
        return {"shard": index}

    across = {"rep": other_rep}
    near = shard(z_near * GROUP + q)
    opposite = shard(z_half * GROUP + q)

    def tokens_of(index):
        return pl.ds(index * tok, tok)

    def keys_of(side):
        return pl.ds(pl.multiple_of(side * half, 128), half)

    def columns(o, index, r):
        start = (order_of[o] * GROUP + index) * (PARTS * unit) + r * unit
        return pl.ds(pl.multiple_of(start, 128), unit)

    def unit_of(r):
        return pl.ds(r * unit, unit)

    copy_lr = pltpu.make_async_copy(lr_ref.at[:, :, rep], lr, load_sem.at[0])
    copy_sg = pltpu.make_async_copy(sg_ref, sg, load_sem.at[1])
    copy_rr = pltpu.make_async_copy(rr_ref, rr, load_sem.at[2])
    copy_g = pltpu.make_async_copy(g_ref, g_all.at[tokens_of(q)], load_sem.at[3])
    copies_x = []
    for o in range(3):
        start = pl.multiple_of((order_of[o] * GROUP + q) * (PARTS * unit), 128)
        copies_x.append(
            pltpu.make_async_copy(
                x_ref.at[:, pl.ds(start, PARTS * unit)], x_all.at[o, tokens_of(q)], x_load.at[o]
            )
        )

    lower = q - q % 2

    def wide_columns(index):
        start = (z * GROUP + index) * (PARTS * unit)
        return pl.ds(pl.multiple_of(start, 128), PARTS * unit)

    own_tokens = pl.ds((q % 2) * tok, tok)
    copies_own = []
    for w, index in enumerate((q, far)):
        copies_own.append(
            pltpu.make_async_copy(
                x_ref.at[:, wide_columns(index)], x_own.at[w, own_tokens], d_load.at[w]
            )
        )

    barrier = pltpu.get_barrier_semaphore()
    peers = [across, near]
    for index in (core, far, both):
        peers.append(shard(base + index))
    inner = jnp.logical_and(z > 0, z < 3)
    facing = shard(z_last * GROUP + q)
    for peer in peers:
        pl.semaphore_signal(barrier, inc=1, device_id=peer, device_id_type=MESH)

    @pl.when(inner)
    def _():
        pl.semaphore_signal(barrier, inc=1, device_id=facing, device_id_type=MESH)

    copy_g.start()
    for copy in copies_own:
        copy.start()
    copy_lr.start()
    copy_sg.start()
    copy_rr.start()
    for copy in copies_x:
        copy.start()
    copy_g.wait()
    @pl.when(inner)
    def _():
        pl.semaphore_wait(barrier, len(peers) + 1)
        pl.semaphore_signal(open_sem, inc=1, device_id=facing, device_id_type=MESH)

    @pl.when(jnp.logical_not(inner))
    def _():
        pl.semaphore_wait(barrier, len(peers))


    def send(src, dst, kind, recv_sem, target):
        remote(src, dst, send_sem.at[kind], recv_sem, target).start()

    def arrive(ref, recv_sem):
        remote(ref, ref, send_sem.at[0], recv_sem, across).wait_recv()

    def send_g(which, target, place):
        keys = keys_of(other_rep if which == 0 else rep)
        view = g_all.at[tokens_of(q), keys]
        send(view, view, 0, g_recv.at[which, place], shard(base + target))

    def send_x(o, r):
        for target in (far, both, core):
            send(
                x_ref.at[:, columns(o, target, r)],
                x_all.at[o, tokens_of(q), unit_of(r)],
                1,
                x_recv.at[o, r],
                shard(base + target),
            )

    send_g(0, far, 0)
    send_g(0, core, 1)
    for w, index in enumerate((core, both)):
        send(
            x_ref.at[:, wide_columns(index)], x_own.at[w, own_tokens], 9, d_recv.at[w],
            shard(base + core),
        )
    send_g(1, core, 1)
    for r in range(PARTS):
        send_x(0, r)
    send_g(1, far, 0)
    for o in (1, 2):
        for r in range(PARTS):
            send_x(o, r)

    pair = pl.ds(lower * tok, 2 * tok)
    mate_tokens = pl.ds((1 - q % 2) * tok, tok)

    def partial_own(w, r, side):
        return lax.dot_general(
            x_own[w, :, r * unit : (r + 1) * unit],
            g_all[pair, keys_of(side)],
            (((0,), (0,)), ((), ())),
            preferred_element_type=jnp.float32,
        )

    def give_own(w, r):
        v = w * PARTS + r
        part_own[v] = partial_own(w, r, other_rep).astype(jnp.bfloat16)
        send(part_own.at[v], met_own.at[v], 10, e_recv.at[v], across)

    def keep_own(w, r):
        kept_own[w * PARTS + r] = partial_own(w, r, rep)

    def total_own(w, r):
        v = w * PARTS + r
        arrive(met_own.at[v], e_recv.at[v])
        return kept_own[v] + met_own[v].astype(jnp.float32)

    def turn(r):
        turned[r] = total_own(1, r).astype(jnp.bfloat16)

    def send_turned(r):
        send(turned.at[r], got.at[r], 11, f_recv.at[r], shard(base + far))

    for which in (0, 1):
        keys = keys_of(other_rep if which == 0 else rep)
        arrive(g_all.at[tokens_of(core), keys], g_recv.at[which, 1])
    for w in range(2):
        copies_own[w].wait()
        arrive(x_own.at[w, mate_tokens], d_recv.at[w])
    for r in range(PARTS):
        give_own(1, r)

    @pl.when(inner)
    def _():
        pl.semaphore_wait(open_sem, 1)
        pl.semaphore_signal(open_sem, inc=1, device_id=near, device_id_type=MESH)

    chosen = jnp.zeros((blocks, 128), jnp.int32)
    row = lax.broadcasted_iota(jnp.int32, (blocks, 128), 0)
    for b in range(blocks):
        chosen = jnp.where(row == b, slot_ref[b], chosen)
    lane = lax.broadcasted_iota(jnp.int32, (blocks, 128), 1)
    per = 4 * slots * height
    for k, index in enumerate(relatives):
        for part_of in range(per // 128):
            place = lane + part_of * 128
            source = place // (slots * height) * (GROUP * slots) + index * slots
            source = source + place // height % slots
            same = source == chosen
            for i in range(height):
                hit = jnp.logical_and(same, place % height == i)
                hot[k, pl.ds(i * blocks, blocks), pl.ds(part_of * 128, 128)] = jnp.where(
                    hit, 1.0, 0.0
                ).astype(jnp.bfloat16)

    copy_lr.wait()
    copy_sg.wait()
    copy_rr.wait()
    for s in range(slots):
        left = jnp.dot(
            lr[s].reshape(n * height, width), sg[s], preferred_element_type=jnp.float32
        ).astype(jnp.bfloat16)
        full = jnp.dot(left, rr[s], preferred_element_type=jnp.float32).astype(jnp.bfloat16)
        prod[:, s] = full.reshape(4, GROUP, height, width)
        if s == 0:

            @pl.when(jnp.logical_not(inner))
            def _():
                pl.semaphore_wait(open_sem, 1)

        for level in (z_last, z_half, z_near):
            send(prod.at[level, s], relay.at[z, s], 2, u_recv.at[0], shard(level * GROUP + q))
    for r in range(PARTS):
        give_own(0, r)
    relay[z] = prod[z]

    def gather_g(which):
        keys = keys_of(other_rep if which == 0 else rep)
        view = g_all.at[tokens_of(far), keys]
        arrive(view, g_recv.at[which, 0])
        send(view, view, 0, g_recv.at[which, 2], shard(base + core))
        arrive(g_all.at[tokens_of(both), keys], g_recv.at[which, 2])

    def partial(o, r, side):
        return lax.dot_general(
            x_all[o, :, r * unit : (r + 1) * unit],
            g_all[:, keys_of(side)],
            (((0,), (0,)), ((), ())),
            preferred_element_type=jnp.float32,
        )

    def give(o, r):
        if r == 0:
            copies_x[o].wait()
        arrive(x_all.at[o, pl.ds(0, 3 * tok), unit_of(r)], x_recv.at[o, r])
        part[o * PARTS + r] = partial(o, r, other_rep).astype(jnp.bfloat16)
        send(
            part.at[o * PARTS + r], met.at[o * PARTS + r], 3, a_recv.at[o * PARTS + r], across
        )

    def keep(o, r):
        kept[o * PARTS + r] = partial(o, r, rep)

    def total_of(o, r):
        u = o * PARTS + r
        arrive(met.at[u], a_recv.at[u])
        return kept[u] + met[u].astype(jnp.float32)

    def pass_near(o, r):
        u = o // 2 * PARTS + r
        passed[u] = total_of(o, r).astype(jnp.bfloat16)
        send(passed.at[u], first.at[u], 4, s_recv.at[u], near)

    def pass_half(r):
        u = 2 * PARTS + r
        total = total_of(1, r)
        arrive(first.at[r], s_recv.at[r])
        passed[u] = (total + first[r].astype(jnp.float32)).astype(jnp.bfloat16)
        send(passed.at[u], second.at[r], 5, t_recv.at[r], opposite)

    def finish(r):
        total = total_own(0, r)
        arrive(got.at[r], f_recv.at[r])
        total = total + got[r].astype(jnp.float32)
        arrive(second.at[r], t_recv.at[r])
        total = total + second[r].astype(jnp.float32)
        arrive(first.at[PARTS + r], s_recv.at[PARTS + r])
        total = total + first[PARTS + r].astype(jnp.float32)
        view = sums.at[rep, unit_of(r)]
        sums[rep, unit_of(r)] = total.astype(jnp.bfloat16)
        send(view, view, 6, r_recv.at[r], across)

    def slice_of(p):
        return pl.ds(p * piece, piece)

    def spread(p):
        for k, target in ((2, far), (3, both), (1, core)):
            send(
                relay.at[:, :, target, :, slice_of(p)],
                upd.at[k, :, :, :, slice_of(p)],
                7,
                y_recv.at[p],
                shard(base + target),
            )

    def select(p):
        cols = slice(p * piece, (p + 1) * piece)
        arrive(upd.at[pl.ds(1, 3), :, :, :, slice_of(p)], y_recv.at[p])
        value = jnp.dot(
            hot[0], relay[:, :, q, :, cols].reshape(per, piece), preferred_element_type=jnp.float32
        )
        for k in range(1, 4):
            value = value + jnp.dot(
                hot[k], upd[k, :, :, :, cols].reshape(per, piece),
                preferred_element_type=jnp.float32,
            )
        rows[rep, :, :, cols] = value.astype(jnp.bfloat16).reshape(height, blocks, piece)
        view = rows.at[rep, :, :, slice_of(p)]
        send(view, view, 8, v_recv.at[p], across)

    outs = []

    def put(src, dst):
        copy = pltpu.make_async_copy(src, dst, out_sem.at[len(outs)])
        copy.start()
        outs.append(copy)

    def widen(side, r):
        wide[unit_of(r), keys_of(side)] = sums[side, unit_of(r)].astype(jnp.float32)
        put(wide.at[unit_of(r), keys_of(side)], og_ref.at[unit_of(r), keys_of(side)])

    for w in (1, 0):
        for r in range(PARTS):
            keep_own(w, r)
    gather_g(0)
    give(0, 0)
    give(0, 1)
    gather_g(1)
    keep(0, 0)
    keep(0, 1)
    pass_near(0, 0)
    give(1, 0)
    keep(1, 0)
    pass_near(0, 1)
    give(1, 1)
    keep(1, 1)
    turn(0)
    turn(1)
    give(2, 0)
    keep(2, 0)
    arrive(relay.at[pl.ds(0, 3)], u_recv.at[0])
    spread(0)
    spread(1)
    send_turned(0)
    send_turned(1)
    spread(2)
    spread(3)
    pass_half(0)
    give(2, 1)
    keep(2, 1)
    pass_half(1)
    pass_near(2, 0)
    select(0)
    pass_near(2, 1)
    select(1)
    finish(0)
    finish(1)
    select(2)
    select(3)
    widen(rep, 0)
    widen(rep, 1)
    put(rows.at[rep], ou_ref.at[rep])
    for r in range(PARTS):
        arrive(sums.at[other_rep, unit_of(r)], r_recv.at[r])
        widen(other_rep, r)
    for p in range(PIECES):
        view = rows.at[other_rep, :, :, slice_of(p)]
        arrive(view, v_recv.at[p])
        put(view, ou_ref.at[other_rep, :, :, slice_of(p)])

    def drain(ref, kind):
        remote(ref, ref, send_sem.at[kind], send_sem.at[kind], across).wait_send()

    drain(x_all, 0)
    drain(x_all.at[:, pl.ds(0, 3 * tok)], 1)
    drain(relay.at[pl.ds(0, 3)], 2)
    drain(met, 3)
    drain(prod.at[0], 9)
    drain(met_own, 10)
    drain(got, 11)
    drain(met.at[pl.ds(0, 2 * PARTS)], 4)
    drain(met.at[pl.ds(0, PARTS)], 5)
    drain(met.at[pl.ds(0, PARTS)], 6)
    drain(relay.at[pl.ds(0, 3)], 7)
    drain(rows.at[0], 8)
    for copy in outs:
        copy.wait()


def fused_shards(tokens_x, key_grad, left_root, slot_grads, right_root, block_slot):
    n = lax.axis_size("shard")
    n_rep = lax.axis_size("rep")
    tok, d_model = tokens_x.shape
    key_width = key_grad.shape[1]
    cols = d_model // n
    slots, order_b, width = left_root.shape
    height = order_b // n // n_rep
    blocks = block_slot.shape[0]
    half = key_width // n_rep
    unit = cols // PARTS
    per = 4 * slots * height
    bf16, f32 = jnp.bfloat16, jnp.float32
    dma = pltpu.SemaphoreType.DMA
    any_spec = pl.BlockSpec(memory_space=pl.ANY)
    sums, rows = pl.pallas_call(
        kernel,
        out_shape=(
            jax.ShapeDtypeStruct((cols, key_width), f32),
            jax.ShapeDtypeStruct((n_rep, height, blocks, width), bf16),
        ),
        in_specs=[pl.BlockSpec(memory_space=pltpu.SMEM)] + [any_spec] * 5,
        out_specs=(any_spec, any_spec),
        scratch_shapes=[
            pltpu.VMEM((3, GROUP * tok, cols), bf16),
            pltpu.VMEM((GROUP * tok, key_width), bf16),
            pltpu.VMEM((slots, n, height, width), bf16),
            pltpu.VMEM(slot_grads.shape, bf16),
            pltpu.VMEM(right_root.shape, bf16),
            pltpu.VMEM((4, slots, GROUP, height, width), bf16),
            pltpu.VMEM((4, slots, GROUP, height, width), bf16),
            pltpu.VMEM((4, 4, slots, height, width), bf16),
            pltpu.VMEM((4, height * blocks, per), bf16),
            pltpu.VMEM((3 * PARTS, unit, half), bf16),
            pltpu.VMEM((3 * PARTS, unit, half), bf16),
            pltpu.VMEM((3 * PARTS, unit, half), f32),
            pltpu.VMEM((3 * PARTS, unit, half), bf16),
            pltpu.VMEM((2 * PARTS, unit, half), bf16),
            pltpu.VMEM((PARTS, unit, half), bf16),
            pltpu.VMEM((2, 2 * tok, cols), bf16),
            pltpu.VMEM((2 * PARTS, unit, half), bf16),
            pltpu.VMEM((2 * PARTS, unit, half), bf16),
            pltpu.VMEM((2 * PARTS, unit, half), f32),
            pltpu.VMEM((PARTS, unit, half), bf16),
            pltpu.VMEM((PARTS, unit, half), bf16),
            pltpu.VMEM((n_rep, cols, half), bf16),
            pltpu.VMEM((n_rep, height, blocks, width), bf16),
            pltpu.VMEM((cols, key_width), f32),
            pltpu.SemaphoreType.REGULAR,
            dma((4,)),
            dma((3,)),
            dma((1 + 2 * PARTS + PIECES,)),
            dma((12,)),
            dma((2, 3)),
            dma((3, PARTS)),
            dma((1,)),
            dma((PIECES,)),
            dma((3 * PARTS,)),
            dma((2 * PARTS,)),
            dma((PARTS,)),
            dma((PARTS,)),
            dma((PIECES,)),
            dma((2,)),
            dma((2,)),
            dma((2 * PARTS,)),
            dma((PARTS,)),
        ],
        compiler_params=pltpu.CompilerParams(
            collective_id=0, has_side_effects=True, vmem_limit_bytes=60 * 1024 * 1024
        ),
    )(
        block_slot,
        tokens_x,
        key_grad,
        left_root.reshape(slots, n, n_rep, height, width),
        slot_grads,
        right_root,
    )
    return (sums, rows.reshape(n_rep * height, blocks, width))


def shards(tokens_x, key_grad, left_root, slot_grads, right_root, block_slot):
    n = lax.axis_size("shard")
    n_rep = lax.axis_size("rep")
    cols = tokens_x.shape[1] // n
    width = left_root.shape[2]
    per = left_root.shape[0] * left_root.shape[1] // (GROUP * n_rep)
    aligned = (
        n_rep == 2
        and n == 4 * GROUP
        and tokens_x.shape[1] % (n * PARTS * 128) == 0
        and key_grad.shape[1] % (n_rep * 128) == 0
        and 2 * key_grad.shape[1] == GROUP * PARTS * cols
        and tokens_x.shape[0] % 16 == 0
        and left_root.shape[1] % (n * n_rep * 16) == 0
        and width % (PIECES * 128) == 0
        and per % 128 == 0
        and block_slot.shape[0] % 16 == 0
    )
    program = fused_shards if aligned else plain_shards
    return program(tokens_x, key_grad, left_root, slot_grads, right_root, block_slot)


def solution(mesh):
    return jax.shard_map(
        shards,
        mesh=mesh,
        in_specs=(
            P(("rep", "shard"), None),
            P(("rep", "shard"), None),
            P("shard", None, None),
            P("shard", None, None),
            P("shard", None, None),
            P(),
        ),
        out_specs=(P("shard", None), P("shard", None, None)),
        check_vma=False,
    )
```

```python
import jax
import jax.numpy as jnp
from jax import lax
from jax.experimental import pallas as pl
from jax.experimental.pallas import tpu as pltpu
from jax.sharding import PartitionSpec as P

MESH = pl.DeviceIdType.MESH
GROUP = 4
PARTS = 2
PIECES = 4


def column_term(features, cotangent):
    return lax.dot_general(
        features, cotangent, (((0,), (0,)), ((), ())), preferred_element_type=jnp.float32
    )


def precondition(left_block, grad_block, right_block):
    left_part = jnp.einsum(
        "sij,sjk->sik", left_block, grad_block, preferred_element_type=jnp.float32
    ).astype(jnp.bfloat16)
    return jnp.einsum(
        "sij,sjk->isk", left_part, right_block, preferred_element_type=jnp.float32
    ).astype(jnp.bfloat16)


def plain_shards(tokens_x, key_grad, left_root, slot_grads, right_root, block_slot):
    n_shard = lax.axis_size("shard")
    n_rep = lax.axis_size("rep")
    own_rows = lax.psum_scatter(
        column_term(tokens_x, key_grad), "shard", scatter_dimension=0, tiled=True
    )
    grad_key = lax.psum(own_rows, "rep")
    slot_count = left_root.shape[0]
    half_slots = slot_count // n_rep
    first_slot = lax.axis_index("rep") * half_slots

    def own_half(values):
        return lax.dynamic_slice_in_dim(values, first_slot, half_slots, 0)

    product = precondition(own_half(left_root), own_half(slot_grads), own_half(right_root))
    received = lax.all_to_all(product, "shard", split_axis=0, concat_axis=1, tiled=True)
    joined = lax.all_gather(received, "rep", axis=1, tiled=True)
    owner = block_slot // slot_count
    within = block_slot % slot_count
    position = (
        within // half_slots * (n_shard * half_slots) + owner * half_slots + within % half_slots
    )
    update = jnp.take(joined, position, axis=1)
    return (grad_key, update)


def remote(src, dst, send_sem, recv_sem, target):
    return pltpu.make_async_remote_copy(
        src_ref=src,
        dst_ref=dst,
        send_sem=send_sem,
        recv_sem=recv_sem,
        device_id=target,
        device_id_type=MESH,
    )


def kernel(
    where_ref, x_ref, g_ref, lr_ref, sg_ref, rr_ref, wide, rows,
    x_all, g_all, lr, sg, rr, prod, relay, upd, hot, part, met, kept, passed, first, second,
    x_own, part_own, met_own, kept_own, turned, got,
    sums, slot_ref,
    open_sem, load_sem, slot_load, x_load, send_sem, g_recv, x_recv, u_recv, y_recv, a_recv, s_recv, t_recv,
    r_recv, v_recv, d_load, d_recv, e_recv, f_recv,
):
    me = lax.axis_index("shard")
    rep = lax.axis_index("rep")
    other_rep = 1 - rep
    q = me % GROUP
    z = me // GROUP
    base = z * GROUP
    core = q + 1 - 2 * (q % 2)
    far = (q + 2) % GROUP
    both = (core + 2) % GROUP
    relatives = (q, core, far, both)
    z_near = z + 1 - 2 * (z % 2)
    z_half = (z + 2) % 4
    z_last = 3 - z
    order_of = (z_last, z_half, z_near, z)
    tok = g_ref.shape[0]
    unit = met.shape[1]
    half = met.shape[2]
    slots = lr.shape[0]
    n = lr.shape[1]
    height = lr.shape[2]
    width = lr.shape[3]
    blocks = slot_ref.shape[0]
    piece = width // PIECES

    def shard(index):
        return {"shard": index}

    across = {"rep": other_rep}
    near = shard(z_near * GROUP + q)
    opposite = shard(z_half * GROUP + q)

    def tokens_of(index):
        return pl.ds(index * tok, tok)

    def keys_of(side):
        return pl.ds(pl.multiple_of(side * half, 128), half)

    def columns(o, index, r):
        start = (order_of[o] * GROUP + index) * (PARTS * unit) + r * unit
        return pl.ds(pl.multiple_of(start, 128), unit)

    def unit_of(r):
        return pl.ds(r * unit, unit)

    copies_slot = []
    for s in range(slots):
        copies_slot.append(
            (
                pltpu.make_async_copy(lr_ref.at[s, :, rep], lr.at[s], slot_load.at[s, 0]),
                pltpu.make_async_copy(sg_ref.at[s], sg.at[s], slot_load.at[s, 1]),
                pltpu.make_async_copy(rr_ref.at[s], rr.at[s], slot_load.at[s, 2]),
            )
        )
    copy_g = pltpu.make_async_copy(g_ref, g_all.at[tokens_of(q)], load_sem.at[0])
    copies_x = []
    for o in range(3):
        start = pl.multiple_of((order_of[o] * GROUP + q) * (PARTS * unit), 128)
        copies_x.append(
            pltpu.make_async_copy(
                x_ref.at[:, pl.ds(start, PARTS * unit)], x_all.at[o, tokens_of(q)], x_load.at[o]
            )
        )

    lower = q - q % 2

    def wide_columns(index):
        start = (z * GROUP + index) * (PARTS * unit)
        return pl.ds(pl.multiple_of(start, 128), PARTS * unit)

    own_tokens = pl.ds((q % 2) * tok, tok)
    copies_own = []
    for w, index in enumerate((q, far)):
        copies_own.append(
            pltpu.make_async_copy(
                x_ref.at[:, wide_columns(index)], x_own.at[w, own_tokens], d_load.at[w]
            )
        )

    copy_g.start()
    barrier = pltpu.get_barrier_semaphore()
    peers = [across, near]
    for index in (core, far, both):
        peers.append(shard(base + index))
    inner = jnp.logical_and(z > 0, z < 3)
    facing = shard(z_last * GROUP + q)
    for peer in peers:
        pl.semaphore_signal(barrier, inc=1, device_id=peer, device_id_type=MESH)

    @pl.when(inner)
    def _():
        pl.semaphore_signal(barrier, inc=1, device_id=facing, device_id_type=MESH)

    copy_slot = pltpu.make_async_copy(where_ref, slot_ref, load_sem.at[1])
    copy_g.wait()
    for copy in copies_slot[0]:
        copy.start()
    for copy in copies_own:
        copy.start()
    for group in copies_slot[1:]:
        for copy in group:
            copy.start()
    for copy in copies_x:
        copy.start()
    copy_slot.start()
    @pl.when(inner)
    def _():
        pl.semaphore_wait(barrier, len(peers) + 1)
        pl.semaphore_signal(open_sem, inc=1, device_id=facing, device_id_type=MESH)

    @pl.when(jnp.logical_not(inner))
    def _():
        pl.semaphore_wait(barrier, len(peers))


    def send(src, dst, kind, recv_sem, target):
        remote(src, dst, send_sem.at[kind], recv_sem, target).start()

    def arrive(ref, recv_sem):
        remote(ref, ref, send_sem.at[0], recv_sem, across).wait_recv()

    def send_g(which, target, place):
        keys = keys_of(other_rep if which == 0 else rep)
        view = g_all.at[tokens_of(q), keys]
        send(view, view, 0, g_recv.at[which, place], shard(base + target))

    def send_x(o, r):
        for target in (far, both, core):
            send(
                x_ref.at[:, columns(o, target, r)],
                x_all.at[o, tokens_of(q), unit_of(r)],
                1,
                x_recv.at[o, r],
                shard(base + target),
            )

    send_g(0, far, 0)
    send_g(0, core, 1)
    for w, index in enumerate((core, both)):
        send(
            x_ref.at[:, wide_columns(index)], x_own.at[w, own_tokens], 9, d_recv.at[w],
            shard(base + core),
        )
    send_g(1, core, 1)
    for r in range(PARTS):
        send_x(0, r)
    send_g(1, far, 0)
    for o in (1, 2):
        for r in range(PARTS):
            send_x(o, r)

    pair = pl.ds(lower * tok, 2 * tok)
    mate_tokens = pl.ds((1 - q % 2) * tok, tok)

    def partial_own(w, r, side):
        return lax.dot_general(
            x_own[w, :, r * unit : (r + 1) * unit],
            g_all[pair, keys_of(side)],
            (((0,), (0,)), ((), ())),
            preferred_element_type=jnp.float32,
        )

    def give_own(w, r):
        v = w * PARTS + r
        part_own[v] = partial_own(w, r, other_rep).astype(jnp.bfloat16)
        send(part_own.at[v], met_own.at[v], 10, e_recv.at[v], across)

    def keep_own(w, r):
        kept_own[w * PARTS + r] = partial_own(w, r, rep)

    def total_own(w, r):
        v = w * PARTS + r
        arrive(met_own.at[v], e_recv.at[v])
        return kept_own[v] + met_own[v].astype(jnp.float32)

    def turn(r):
        turned[r] = total_own(1, r).astype(jnp.bfloat16)

    def send_turned(r):
        send(turned.at[r], got.at[r], 11, f_recv.at[r], shard(base + far))

    def send_slot(s, levels):
        for level in levels:
            send(prod.at[level, s], relay.at[z, s], 2, u_recv.at[0], shard(level * GROUP + q))

    for s in range(slots):
        for copy in copies_slot[s]:
            copy.wait()
        left = jnp.dot(
            lr[s].reshape(n * height, width), sg[s], preferred_element_type=jnp.float32
        ).astype(jnp.bfloat16)
        full = jnp.dot(left, rr[s], preferred_element_type=jnp.float32).astype(jnp.bfloat16)
        prod[:, s] = full.reshape(4, GROUP, height, width)
        if s == 0:

            @pl.when(inner)
            def _():
                pl.semaphore_wait(open_sem, 1)
                pl.semaphore_signal(open_sem, inc=1, device_id=near, device_id_type=MESH)

            send_slot(s, (z_near,))
        elif s == 1:

            @pl.when(jnp.logical_not(inner))
            def _():
                pl.semaphore_wait(open_sem, 1)

            send_slot(0, (z_last, z_half))
            send_slot(1, (z_last, z_half, z_near))
        else:
            send_slot(s, (z_last, z_half, z_near))

    arrive(g_all.at[tokens_of(core), keys_of(other_rep)], g_recv.at[0, 1])
    for w in range(2):
        copies_own[w].wait()
        arrive(x_own.at[w, mate_tokens], d_recv.at[w])
    for r in range(PARTS):
        give_own(1, r)

    copy_slot.wait()
    chosen = jnp.zeros((blocks, 128), jnp.int32)
    row = lax.broadcasted_iota(jnp.int32, (blocks, 128), 0)
    for b in range(blocks):
        chosen = jnp.where(row == b, slot_ref[b], chosen)
    lane = lax.broadcasted_iota(jnp.int32, (blocks, 128), 1)
    per = 4 * slots * height
    for k, index in enumerate(relatives):
        for part_of in range(per // 128):
            place = lane + part_of * 128
            source = place // (slots * height) * (GROUP * slots) + index * slots
            source = source + place // height % slots
            same = source == chosen
            for i in range(height):
                hit = jnp.logical_and(same, place % height == i)
                hot[k, pl.ds(i * blocks, blocks), pl.ds(part_of * 128, 128)] = jnp.where(
                    hit, 1.0, 0.0
                ).astype(jnp.bfloat16)

    for r in range(PARTS):
        give_own(0, r)
    relay[z] = prod[z]

    def gather_g(which):
        keys = keys_of(other_rep if which == 0 else rep)
        view = g_all.at[tokens_of(far), keys]
        arrive(view, g_recv.at[which, 0])
        send(view, view, 0, g_recv.at[which, 2], shard(base + core))
        arrive(g_all.at[tokens_of(both), keys], g_recv.at[which, 2])

    def partial(o, r, side):
        return lax.dot_general(
            x_all[o, :, r * unit : (r + 1) * unit],
            g_all[:, keys_of(side)],
            (((0,), (0,)), ((), ())),
            preferred_element_type=jnp.float32,
        )

    def give(o, r):
        if r == 0:
            copies_x[o].wait()
        arrive(x_all.at[o, pl.ds(0, 3 * tok), unit_of(r)], x_recv.at[o, r])
        part[o * PARTS + r] = partial(o, r, other_rep).astype(jnp.bfloat16)
        send(
            part.at[o * PARTS + r], met.at[o * PARTS + r], 3, a_recv.at[o * PARTS + r], across
        )

    def keep(o, r):
        kept[o * PARTS + r] = partial(o, r, rep)

    def total_of(o, r):
        u = o * PARTS + r
        arrive(met.at[u], a_recv.at[u])
        return kept[u] + met[u].astype(jnp.float32)

    def pass_near(o, r):
        u = o // 2 * PARTS + r
        passed[u] = total_of(o, r).astype(jnp.bfloat16)
        send(passed.at[u], first.at[u], 4, s_recv.at[u], near)

    def pass_half(r):
        u = 2 * PARTS + r
        total = total_of(1, r)
        arrive(first.at[r], s_recv.at[r])
        passed[u] = (total + first[r].astype(jnp.float32)).astype(jnp.bfloat16)
        send(passed.at[u], second.at[r], 5, t_recv.at[r], opposite)

    def finish(r):
        total = total_own(0, r)
        arrive(got.at[r], f_recv.at[r])
        total = total + got[r].astype(jnp.float32)
        arrive(second.at[r], t_recv.at[r])
        total = total + second[r].astype(jnp.float32)
        arrive(first.at[PARTS + r], s_recv.at[PARTS + r])
        total = total + first[PARTS + r].astype(jnp.float32)
        view = sums.at[rep, unit_of(r)]
        sums[rep, unit_of(r)] = total.astype(jnp.bfloat16)
        send(view, view, 6, r_recv.at[r], across)

    def slice_of(p):
        return pl.ds(p * piece, piece)

    def spread(p):
        for k, target in ((2, far), (3, both), (1, core)):
            send(
                relay.at[:, :, target, :, slice_of(p)],
                upd.at[k, :, :, :, slice_of(p)],
                7,
                y_recv.at[p],
                shard(base + target),
            )

    def select(p):
        cols = slice(p * piece, (p + 1) * piece)
        arrive(upd.at[pl.ds(1, 3), :, :, :, slice_of(p)], y_recv.at[p])
        value = jnp.dot(
            hot[0], relay[:, :, q, :, cols].reshape(per, piece), preferred_element_type=jnp.float32
        )
        for k in range(1, 4):
            value = value + jnp.dot(
                hot[k], upd[k, :, :, :, cols].reshape(per, piece),
                preferred_element_type=jnp.float32,
            )
        rows[rep, :, :, cols] = value.astype(jnp.bfloat16).reshape(height, blocks, piece)
        view = rows.at[rep, :, :, slice_of(p)]
        send(view, view, 8, v_recv.at[p], across)

    def widen(side, r):
        wide[unit_of(r), keys_of(side)] = sums[side, unit_of(r)].astype(jnp.float32)

    arrive(g_all.at[tokens_of(core), keys_of(rep)], g_recv.at[1, 1])
    for w in (1, 0):
        for r in range(PARTS):
            keep_own(w, r)
    gather_g(0)
    give(0, 0)
    give(0, 1)
    gather_g(1)
    keep(0, 0)
    keep(0, 1)
    pass_near(0, 0)
    give(1, 0)
    keep(1, 0)
    pass_near(0, 1)
    give(1, 1)
    keep(1, 1)
    turn(0)
    turn(1)
    give(2, 0)
    keep(2, 0)
    arrive(relay.at[pl.ds(0, 3)], u_recv.at[0])
    spread(0)
    spread(1)
    spread(2)
    send_turned(0)
    send_turned(1)
    spread(3)
    pass_half(0)
    give(2, 1)
    keep(2, 1)
    pass_half(1)
    pass_near(2, 0)
    select(0)
    pass_near(2, 1)
    select(1)
    select(2)
    finish(0)
    finish(1)
    select(3)
    widen(rep, 0)
    widen(rep, 1)
    for r in range(PARTS):
        arrive(sums.at[other_rep, unit_of(r)], r_recv.at[r])
        widen(other_rep, r)
    for p in range(PIECES):
        view = rows.at[other_rep, :, :, slice_of(p)]
        arrive(view, v_recv.at[p])

    def drain(ref, kind):
        remote(ref, ref, send_sem.at[kind], send_sem.at[kind], across).wait_send()

    drain(x_all, 0)
    drain(x_all.at[:, pl.ds(0, 3 * tok)], 1)
    drain(relay.at[pl.ds(0, 3)], 2)
    drain(met, 3)
    drain(prod.at[0], 9)
    drain(met_own, 10)
    drain(got, 11)
    drain(met.at[pl.ds(0, 2 * PARTS)], 4)
    drain(met.at[pl.ds(0, PARTS)], 5)
    drain(met.at[pl.ds(0, PARTS)], 6)
    drain(relay.at[pl.ds(0, 3)], 7)
    drain(rows.at[0], 8)


def in_hbm(array):
    return pltpu.with_memory_space_constraint(array, pltpu.HBM)


def in_vmem(array):
    return pltpu.with_memory_space_constraint(array, pltpu.VMEM)


def store(sums_ref, rows_ref, og_ref, ou_ref, sem):
    copies = (
        pltpu.make_async_copy(sums_ref, og_ref, sem.at[0]),
        pltpu.make_async_copy(rows_ref, ou_ref, sem.at[1]),
    )
    for copy in copies:
        copy.start()
    for copy in copies:
        copy.wait()


def fused_shards(tokens_x, key_grad, left_root, slot_grads, right_root, block_slot):
    n = lax.axis_size("shard")
    n_rep = lax.axis_size("rep")
    tok, d_model = tokens_x.shape
    key_width = key_grad.shape[1]
    cols = d_model // n
    slots, order_b, width = left_root.shape
    height = order_b // n // n_rep
    blocks = block_slot.shape[0]
    half = key_width // n_rep
    unit = cols // PARTS
    per = 4 * slots * height
    bf16, f32 = jnp.bfloat16, jnp.float32
    dma = pltpu.SemaphoreType.DMA
    hbm_spec = pl.BlockSpec(memory_space=pltpu.HBM)
    vmem_spec = pl.BlockSpec(memory_space=pltpu.VMEM)
    sums, rows = pl.pallas_call(
        kernel,
        out_shape=(
            pltpu.VMEM((cols, key_width), f32),
            pltpu.VMEM((n_rep, height, blocks, width), bf16),
        ),
        in_specs=[hbm_spec] * 6,
        out_specs=(vmem_spec, vmem_spec),
        scratch_shapes=[
            pltpu.VMEM((3, GROUP * tok, cols), bf16),
            pltpu.VMEM((GROUP * tok, key_width), bf16),
            pltpu.VMEM((slots, n, height, width), bf16),
            pltpu.VMEM(slot_grads.shape, bf16),
            pltpu.VMEM(right_root.shape, bf16),
            pltpu.VMEM((4, slots, GROUP, height, width), bf16),
            pltpu.VMEM((4, slots, GROUP, height, width), bf16),
            pltpu.VMEM((4, 4, slots, height, width), bf16),
            pltpu.VMEM((4, height * blocks, per), bf16),
            pltpu.VMEM((3 * PARTS, unit, half), bf16),
            pltpu.VMEM((3 * PARTS, unit, half), bf16),
            pltpu.VMEM((3 * PARTS, unit, half), f32),
            pltpu.VMEM((3 * PARTS, unit, half), bf16),
            pltpu.VMEM((2 * PARTS, unit, half), bf16),
            pltpu.VMEM((PARTS, unit, half), bf16),
            pltpu.VMEM((2, 2 * tok, cols), bf16),
            pltpu.VMEM((2 * PARTS, unit, half), bf16),
            pltpu.VMEM((2 * PARTS, unit, half), bf16),
            pltpu.VMEM((2 * PARTS, unit, half), f32),
            pltpu.VMEM((PARTS, unit, half), bf16),
            pltpu.VMEM((PARTS, unit, half), bf16),
            pltpu.VMEM((n_rep, cols, half), bf16),
            pltpu.SMEM(block_slot.shape, jnp.int32),
            pltpu.SemaphoreType.REGULAR,
            dma((2,)),
            dma((slots, 3)),
            dma((3,)),
            dma((12,)),
            dma((2, 3)),
            dma((3, PARTS)),
            dma((1,)),
            dma((PIECES,)),
            dma((3 * PARTS,)),
            dma((2 * PARTS,)),
            dma((PARTS,)),
            dma((PARTS,)),
            dma((PIECES,)),
            dma((2,)),
            dma((2,)),
            dma((2 * PARTS,)),
            dma((PARTS,)),
        ],
        compiler_params=pltpu.CompilerParams(
            collective_id=0, has_side_effects=True, vmem_limit_bytes=48 * 1024 * 1024
        ),
    )(
        in_hbm(block_slot),
        in_hbm(tokens_x),
        in_hbm(key_grad),
        in_hbm(left_root.reshape(slots, n, n_rep, height, width)),
        in_hbm(slot_grads),
        in_hbm(right_root),
    )
    rows = rows.reshape(n_rep * height, blocks, width)
    return pl.pallas_call(
        store,
        out_shape=(
            jax.ShapeDtypeStruct(sums.shape, sums.dtype),
            jax.ShapeDtypeStruct(rows.shape, rows.dtype),
        ),
        in_specs=[vmem_spec, vmem_spec],
        out_specs=(hbm_spec, hbm_spec),
        scratch_shapes=[dma((2,))],
    )(in_vmem(sums), in_vmem(rows))


def shards(tokens_x, key_grad, left_root, slot_grads, right_root, block_slot):
    n = lax.axis_size("shard")
    n_rep = lax.axis_size("rep")
    cols = tokens_x.shape[1] // n
    width = left_root.shape[2]
    per = left_root.shape[0] * left_root.shape[1] // (GROUP * n_rep)
    aligned = (
        n_rep == 2
        and n == 4 * GROUP
        and tokens_x.shape[1] % (n * PARTS * 128) == 0
        and key_grad.shape[1] % (n_rep * 128) == 0
        and 2 * key_grad.shape[1] == GROUP * PARTS * cols
        and tokens_x.shape[0] % 16 == 0
        and left_root.shape[1] % (n * n_rep * 16) == 0
        and width % (PIECES * 128) == 0
        and per % 128 == 0
        and block_slot.shape[0] % 16 == 0
        and left_root.shape[0] > 1
    )
    program = fused_shards if aligned else plain_shards
    return program(tokens_x, key_grad, left_root, slot_grads, right_root, block_slot)


def solution(mesh):
    return jax.shard_map(
        shards,
        mesh=mesh,
        in_specs=(
            P(("rep", "shard"), None),
            P(("rep", "shard"), None),
            P("shard", None, None),
            P("shard", None, None),
            P("shard", None, None),
            P(),
        ),
        out_specs=(P("shard", None), P("shard", None, None)),
        check_vma=False,
    )
```

```python
import jax
import jax.numpy as jnp
from jax import lax
from jax.experimental import pallas as pl
from jax.experimental.pallas import tpu as pltpu
from jax.sharding import PartitionSpec as P

MESH = pl.DeviceIdType.MESH
GROUP = 4
PARTS = 2
PIECES = 4
HALVES = 2


def column_term(features, cotangent):
    return lax.dot_general(
        features, cotangent, (((0,), (0,)), ((), ())), preferred_element_type=jnp.float32
    )


def precondition(left_block, grad_block, right_block):
    left_part = jnp.einsum(
        "sij,sjk->sik", left_block, grad_block, preferred_element_type=jnp.float32
    ).astype(jnp.bfloat16)
    return jnp.einsum(
        "sij,sjk->isk", left_part, right_block, preferred_element_type=jnp.float32
    ).astype(jnp.bfloat16)


def plain_shards(tokens_x, key_grad, left_root, slot_grads, right_root, block_slot):
    n_shard = lax.axis_size("shard")
    n_rep = lax.axis_size("rep")
    own_rows = lax.psum_scatter(
        column_term(tokens_x, key_grad), "shard", scatter_dimension=0, tiled=True
    )
    grad_key = lax.psum(own_rows, "rep")
    slot_count = left_root.shape[0]
    half_slots = slot_count // n_rep
    first_slot = lax.axis_index("rep") * half_slots

    def own_half(values):
        return lax.dynamic_slice_in_dim(values, first_slot, half_slots, 0)

    product = precondition(own_half(left_root), own_half(slot_grads), own_half(right_root))
    received = lax.all_to_all(product, "shard", split_axis=0, concat_axis=1, tiled=True)
    joined = lax.all_gather(received, "rep", axis=1, tiled=True)
    owner = block_slot // slot_count
    within = block_slot % slot_count
    position = (
        within // half_slots * (n_shard * half_slots) + owner * half_slots + within % half_slots
    )
    update = jnp.take(joined, position, axis=1)
    return (grad_key, update)


def remote(src, dst, send_sem, recv_sem, target):
    return pltpu.make_async_remote_copy(
        src_ref=src,
        dst_ref=dst,
        send_sem=send_sem,
        recv_sem=recv_sem,
        device_id=target,
        device_id_type=MESH,
    )


def kernel(
    where_ref, x_ref, g_ref, lr_ref, sg_ref, rr_ref, wide, rows,
    x_all, g_all, lr, sg, rr, prod, relay, upd, hot, part, met, kept, passed, first, second,
    x_own, part_own, met_own, kept_own, turned, got,
    sums, slot_ref,
    open_sem, load_sem, slot_load, x_load, send_sem, g_recv, x_recv, u_recv, y_recv, a_recv, s_recv, t_recv,
    r_recv, v_recv, d_load, d_recv, e_recv, f_recv,
):
    me = lax.axis_index("shard")
    rep = lax.axis_index("rep")
    other_rep = 1 - rep
    q = me % GROUP
    z = me // GROUP
    base = z * GROUP
    core = q + 1 - 2 * (q % 2)
    far = (q + 2) % GROUP
    both = (core + 2) % GROUP
    relatives = (q, core, far, both)
    z_near = z + 1 - 2 * (z % 2)
    z_half = (z + 2) % 4
    z_last = 3 - z
    order_of = (z_last, z_half, z_near, z)
    tok = g_ref.shape[0]
    unit = met.shape[1]
    half = met.shape[2]
    slots = lr.shape[0]
    n = lr.shape[1]
    height = lr.shape[2]
    width = lr.shape[3]
    blocks = slot_ref.shape[0]
    piece = width // PIECES

    def shard(index):
        return {"shard": index}

    across = {"rep": other_rep}
    near = shard(z_near * GROUP + q)
    opposite = shard(z_half * GROUP + q)

    def tokens_of(index):
        return pl.ds(index * tok, tok)

    def keys_of(side):
        return pl.ds(pl.multiple_of(side * half, 128), half)

    def columns(o, index, r):
        start = (order_of[o] * GROUP + index) * (PARTS * unit) + r * unit
        return pl.ds(pl.multiple_of(start, 128), unit)

    def unit_of(r):
        return pl.ds(r * unit, unit)

    copies_slot = []
    for s in range(slots):
        copies_slot.append(
            (
                pltpu.make_async_copy(lr_ref.at[s, :, rep], lr.at[s], slot_load.at[s, 0]),
                pltpu.make_async_copy(sg_ref.at[s], sg.at[s], slot_load.at[s, 1]),
                pltpu.make_async_copy(rr_ref.at[s], rr.at[s], slot_load.at[s, 2]),
            )
        )
    copy_g = pltpu.make_async_copy(g_ref, g_all.at[tokens_of(q)], load_sem.at[0])
    copies_x = []
    for o in range(3):
        start = pl.multiple_of((order_of[o] * GROUP + q) * (PARTS * unit), 128)
        copies_x.append(
            pltpu.make_async_copy(
                x_ref.at[:, pl.ds(start, PARTS * unit)], x_all.at[o, tokens_of(q)], x_load.at[o]
            )
        )

    lower = q - q % 2

    def wide_columns(index):
        start = (z * GROUP + index) * (PARTS * unit)
        return pl.ds(pl.multiple_of(start, 128), PARTS * unit)

    own_tokens = pl.ds((q % 2) * tok, tok)
    copies_own = []
    for w, index in enumerate((q, far)):
        copies_own.append(
            pltpu.make_async_copy(
                x_ref.at[:, wide_columns(index)], x_own.at[w, own_tokens], d_load.at[w]
            )
        )

    copy_g.start()
    barrier = pltpu.get_barrier_semaphore()
    peers = [across, near]
    for index in (core, far, both):
        peers.append(shard(base + index))
    inner = jnp.logical_and(z > 0, z < 3)
    facing = shard(z_last * GROUP + q)
    for peer in peers:
        pl.semaphore_signal(barrier, inc=1, device_id=peer, device_id_type=MESH)

    @pl.when(inner)
    def _():
        pl.semaphore_signal(barrier, inc=1, device_id=facing, device_id_type=MESH)

    copy_slot = pltpu.make_async_copy(where_ref, slot_ref, load_sem.at[1])
    copy_g.wait()
    for copy in copies_slot[0]:
        copy.start()
    for copy in copies_own:
        copy.start()
    for group in copies_slot[1:]:
        for copy in group:
            copy.start()
    for copy in copies_x:
        copy.start()
    copy_slot.start()
    @pl.when(inner)
    def _():
        pl.semaphore_wait(barrier, len(peers) + 1)
        pl.semaphore_signal(open_sem, inc=1, device_id=facing, device_id_type=MESH)

    @pl.when(jnp.logical_not(inner))
    def _():
        pl.semaphore_wait(barrier, len(peers))


    def send(src, dst, kind, recv_sem, target):
        remote(src, dst, send_sem.at[kind], recv_sem, target).start()

    def arrive(ref, recv_sem):
        remote(ref, ref, send_sem.at[0], recv_sem, across).wait_recv()

    def send_g(which, target, place):
        keys = keys_of(other_rep if which == 0 else rep)
        view = g_all.at[tokens_of(q), keys]
        send(view, view, 0, g_recv.at[which, place], shard(base + target))

    def send_x(o, r):
        for target in (far, both, core):
            send(
                x_ref.at[:, columns(o, target, r)],
                x_all.at[o, tokens_of(q), unit_of(r)],
                1,
                x_recv.at[o, r],
                shard(base + target),
            )

    send_g(0, far, 0)
    send_g(0, core, 1)
    for w, index in enumerate((core, both)):
        send(
            x_ref.at[:, wide_columns(index)], x_own.at[w, own_tokens], 9, d_recv.at[w],
            shard(base + core),
        )
    send_g(1, core, 1)
    for r in range(PARTS):
        send_x(0, r)
    send_g(1, far, 0)
    for o in (1, 2):
        for r in range(PARTS):
            send_x(o, r)

    pair = pl.ds(lower * tok, 2 * tok)
    mate_tokens = pl.ds((1 - q % 2) * tok, tok)

    def partial_own(w, r, side):
        return lax.dot_general(
            x_own[w, :, r * unit : (r + 1) * unit],
            g_all[pair, keys_of(side)],
            (((0,), (0,)), ((), ())),
            preferred_element_type=jnp.float32,
        )

    def give_own(w, r):
        v = w * PARTS + r
        part_own[v] = partial_own(w, r, other_rep).astype(jnp.bfloat16)
        send(part_own.at[v], met_own.at[v], 10, e_recv.at[v], across)

    def keep_own(w, r):
        kept_own[w * PARTS + r] = partial_own(w, r, rep)

    def total_own(w, r):
        v = w * PARTS + r
        arrive(met_own.at[v], e_recv.at[v])
        return kept_own[v] + met_own[v].astype(jnp.float32)

    def turn(r):
        turned[r] = total_own(1, r).astype(jnp.bfloat16)

    def send_turned(r):
        send(turned.at[r], got.at[r], 11, f_recv.at[r], shard(base + far))

    def send_slot(s, levels):
        for level in levels:
            send(prod.at[level, s], relay.at[z, s], 2, u_recv.at[0], shard(level * GROUP + q))

    for s in range(slots):
        for copy in copies_slot[s]:
            copy.wait()
        left = jnp.dot(
            lr[s].reshape(n * height, width), sg[s], preferred_element_type=jnp.float32
        ).astype(jnp.bfloat16)
        full = jnp.dot(left, rr[s], preferred_element_type=jnp.float32).astype(jnp.bfloat16)
        prod[:, s] = full.reshape(4, GROUP, height, width)
        if s == 0:

            @pl.when(inner)
            def _():
                pl.semaphore_wait(open_sem, 1)
                pl.semaphore_signal(open_sem, inc=1, device_id=near, device_id_type=MESH)

            send_slot(s, (z_near,))
        elif s == 1:

            @pl.when(jnp.logical_not(inner))
            def _():
                pl.semaphore_wait(open_sem, 1)

            send_slot(0, (z_last, z_half))
            send_slot(1, (z_last, z_half, z_near))
        else:
            send_slot(s, (z_last, z_half, z_near))

    arrive(g_all.at[tokens_of(core), keys_of(other_rep)], g_recv.at[0, 1])
    for w in range(2):
        copies_own[w].wait()
        arrive(x_own.at[w, mate_tokens], d_recv.at[w])
    for r in range(PARTS):
        give_own(1, r)

    copy_slot.wait()
    chosen = jnp.zeros((blocks, 128), jnp.int32)
    row = lax.broadcasted_iota(jnp.int32, (blocks, 128), 0)
    for b in range(blocks):
        chosen = jnp.where(row == b, slot_ref[b], chosen)
    lane = lax.broadcasted_iota(jnp.int32, (blocks, 128), 1)
    per = 4 * slots * height
    for k, index in enumerate(relatives):
        for part_of in range(per // 128):
            place = lane + part_of * 128
            source = place // (slots * height) * (GROUP * slots) + index * slots
            source = source + place // height % slots
            same = source == chosen
            for i in range(height):
                hit = jnp.logical_and(same, place % height == i)
                hot[k, pl.ds(i * blocks, blocks), pl.ds(part_of * 128, 128)] = jnp.where(
                    hit, 1.0, 0.0
                ).astype(jnp.bfloat16)

    for r in range(PARTS):
        give_own(0, r)
    relay[z] = prod[z]

    def gather_g(which):
        keys = keys_of(other_rep if which == 0 else rep)
        view = g_all.at[tokens_of(far), keys]
        arrive(view, g_recv.at[which, 0])
        send(view, view, 0, g_recv.at[which, 2], shard(base + core))
        arrive(g_all.at[tokens_of(both), keys], g_recv.at[which, 2])

    def partial(o, r, side):
        return lax.dot_general(
            x_all[o, :, r * unit : (r + 1) * unit],
            g_all[:, keys_of(side)],
            (((0,), (0,)), ((), ())),
            preferred_element_type=jnp.float32,
        )

    def give(o, r):
        if r == 0:
            copies_x[o].wait()
        arrive(x_all.at[o, pl.ds(0, 3 * tok), unit_of(r)], x_recv.at[o, r])
        part[o * PARTS + r] = partial(o, r, other_rep).astype(jnp.bfloat16)
        send(
            part.at[o * PARTS + r], met.at[o * PARTS + r], 3, a_recv.at[o * PARTS + r], across
        )

    def keep(o, r):
        kept[o * PARTS + r] = partial(o, r, rep)

    def total_of(o, r):
        u = o * PARTS + r
        arrive(met.at[u], a_recv.at[u])
        return kept[u] + met[u].astype(jnp.float32)

    def pass_near(o, r):
        u = o // 2 * PARTS + r
        passed[u] = total_of(o, r).astype(jnp.bfloat16)
        send(passed.at[u], first.at[u], 4, s_recv.at[u], near)

    def pass_half(r):
        u = 2 * PARTS + r
        total = total_of(1, r)
        arrive(first.at[r], s_recv.at[r])
        passed[u] = (total + first[r].astype(jnp.float32)).astype(jnp.bfloat16)
        send(passed.at[u], second.at[r], 5, t_recv.at[r], opposite)

    def finish(r):
        total = total_own(0, r)
        arrive(got.at[r], f_recv.at[r])
        total = total + got[r].astype(jnp.float32)
        arrive(second.at[r], t_recv.at[r])
        total = total + second[r].astype(jnp.float32)
        arrive(first.at[PARTS + r], s_recv.at[PARTS + r])
        total = total + first[PARTS + r].astype(jnp.float32)
        view = sums.at[rep, unit_of(r)]
        sums[rep, unit_of(r)] = total.astype(jnp.bfloat16)
        send(view, view, 6, r_recv.at[r], across)

    def slice_of(p):
        return pl.ds(p * piece, piece)

    def spread(p):
        for k, target in ((2, far), (3, both), (1, core)):
            send(
                relay.at[:, :, target, :, slice_of(p)],
                upd.at[k, :, :, :, slice_of(p)],
                7,
                y_recv.at[k // 2, p],
                shard(base + target),
            )

    lines = height // HALVES

    def select(p):
        cols = slice(p * piece, (p + 1) * piece)

        def block(k):
            return upd[k, :, :, :, cols].reshape(per, piece)

        arrive(upd.at[1, :, :, :, slice_of(p)], y_recv.at[0, p])
        early = jnp.dot(
            hot[0], relay[:, :, q, :, cols].reshape(per, piece), preferred_element_type=jnp.float32
        ) + jnp.dot(hot[1], block(1), preferred_element_type=jnp.float32)
        arrive(upd.at[pl.ds(2, 2), :, :, :, slice_of(p)], y_recv.at[1, p])
        for h in range(HALVES):
            here = slice(h * lines * blocks, (h + 1) * lines * blocks)
            value = early[here]
            for k in (2, 3):
                value = value + jnp.dot(
                    hot[k, here], block(k), preferred_element_type=jnp.float32
                )
            rows[rep, h * lines : (h + 1) * lines, :, cols] = value.astype(jnp.bfloat16).reshape(
                lines, blocks, piece
            )
            view = rows.at[rep, pl.ds(h * lines, lines), :, slice_of(p)]
            send(view, view, 8, v_recv.at[p, h], across)

    def widen(side, r):
        wide[unit_of(r), keys_of(side)] = sums[side, unit_of(r)].astype(jnp.float32)

    arrive(g_all.at[tokens_of(core), keys_of(rep)], g_recv.at[1, 1])
    for w in (1, 0):
        for r in range(PARTS):
            keep_own(w, r)
    gather_g(0)
    give(0, 0)
    give(0, 1)
    gather_g(1)
    keep(0, 0)
    keep(0, 1)
    pass_near(0, 0)
    give(1, 0)
    keep(1, 0)
    pass_near(0, 1)
    give(1, 1)
    keep(1, 1)
    turn(0)
    turn(1)
    give(2, 0)
    keep(2, 0)
    arrive(relay.at[pl.ds(0, 3)], u_recv.at[0])
    spread(0)
    spread(1)
    spread(2)
    send_turned(0)
    spread(3)
    send_turned(1)
    pass_half(0)
    give(2, 1)
    keep(2, 1)
    pass_half(1)
    pass_near(2, 0)
    select(0)
    pass_near(2, 1)
    select(1)
    select(2)
    finish(0)
    select(3)
    finish(1)
    widen(rep, 0)
    widen(rep, 1)
    for r in range(PARTS):
        arrive(sums.at[other_rep, unit_of(r)], r_recv.at[r])
        widen(other_rep, r)
    for p in range(PIECES):
        for h in range(HALVES):
            arrive(
                rows.at[other_rep, pl.ds(h * lines, lines), :, slice_of(p)], v_recv.at[p, h]
            )

    def drain(ref, kind):
        remote(ref, ref, send_sem.at[kind], send_sem.at[kind], across).wait_send()

    drain(x_all, 0)
    drain(x_all.at[:, pl.ds(0, 3 * tok)], 1)
    drain(relay.at[pl.ds(0, 3)], 2)
    drain(met, 3)
    drain(prod.at[0], 9)
    drain(met_own, 10)
    drain(got, 11)
    drain(met.at[pl.ds(0, 2 * PARTS)], 4)
    drain(met.at[pl.ds(0, PARTS)], 5)
    drain(met.at[pl.ds(0, PARTS)], 6)
    drain(relay.at[pl.ds(0, 3)], 7)
    drain(rows.at[0], 8)


def in_hbm(array):
    return pltpu.with_memory_space_constraint(array, pltpu.HBM)


def in_vmem(array):
    return pltpu.with_memory_space_constraint(array, pltpu.VMEM)


def store(sums_ref, rows_ref, og_ref, ou_ref, sem):
    copies = (
        pltpu.make_async_copy(sums_ref, og_ref, sem.at[0]),
        pltpu.make_async_copy(rows_ref, ou_ref, sem.at[1]),
    )
    for copy in copies:
        copy.start()
    for copy in copies:
        copy.wait()


def fused_shards(tokens_x, key_grad, left_root, slot_grads, right_root, block_slot):
    n = lax.axis_size("shard")
    n_rep = lax.axis_size("rep")
    tok, d_model = tokens_x.shape
    key_width = key_grad.shape[1]
    cols = d_model // n
    slots, order_b, width = left_root.shape
    height = order_b // n // n_rep
    blocks = block_slot.shape[0]
    half = key_width // n_rep
    unit = cols // PARTS
    per = 4 * slots * height
    bf16, f32 = jnp.bfloat16, jnp.float32
    dma = pltpu.SemaphoreType.DMA
    hbm_spec = pl.BlockSpec(memory_space=pltpu.HBM)
    vmem_spec = pl.BlockSpec(memory_space=pltpu.VMEM)
    sums, rows = pl.pallas_call(
        kernel,
        out_shape=(
            pltpu.VMEM((cols, key_width), f32),
            pltpu.VMEM((n_rep, height, blocks, width), bf16),
        ),
        in_specs=[hbm_spec] * 6,
        out_specs=(vmem_spec, vmem_spec),
        scratch_shapes=[
            pltpu.VMEM((3, GROUP * tok, cols), bf16),
            pltpu.VMEM((GROUP * tok, key_width), bf16),
            pltpu.VMEM((slots, n, height, width), bf16),
            pltpu.VMEM(slot_grads.shape, bf16),
            pltpu.VMEM(right_root.shape, bf16),
            pltpu.VMEM((4, slots, GROUP, height, width), bf16),
            pltpu.VMEM((4, slots, GROUP, height, width), bf16),
            pltpu.VMEM((4, 4, slots, height, width), bf16),
            pltpu.VMEM((4, height * blocks, per), bf16),
            pltpu.VMEM((3 * PARTS, unit, half), bf16),
            pltpu.VMEM((3 * PARTS, unit, half), bf16),
            pltpu.VMEM((3 * PARTS, unit, half), f32),
            pltpu.VMEM((3 * PARTS, unit, half), bf16),
            pltpu.VMEM((2 * PARTS, unit, half), bf16),
            pltpu.VMEM((PARTS, unit, half), bf16),
            pltpu.VMEM((2, 2 * tok, cols), bf16),
            pltpu.VMEM((2 * PARTS, unit, half), bf16),
            pltpu.VMEM((2 * PARTS, unit, half), bf16),
            pltpu.VMEM((2 * PARTS, unit, half), f32),
            pltpu.VMEM((PARTS, unit, half), bf16),
            pltpu.VMEM((PARTS, unit, half), bf16),
            pltpu.VMEM((n_rep, cols, half), bf16),
            pltpu.SMEM(block_slot.shape, jnp.int32),
            pltpu.SemaphoreType.REGULAR,
            dma((2,)),
            dma((slots, 3)),
            dma((3,)),
            dma((12,)),
            dma((2, 3)),
            dma((3, PARTS)),
            dma((1,)),
            dma((2, PIECES)),
            dma((3 * PARTS,)),
            dma((2 * PARTS,)),
            dma((PARTS,)),
            dma((PARTS,)),
            dma((PIECES, HALVES)),
            dma((2,)),
            dma((2,)),
            dma((2 * PARTS,)),
            dma((PARTS,)),
        ],
        compiler_params=pltpu.CompilerParams(
            collective_id=0, has_side_effects=True, vmem_limit_bytes=48 * 1024 * 1024
        ),
    )(
        in_hbm(block_slot),
        in_hbm(tokens_x),
        in_hbm(key_grad),
        in_hbm(left_root.reshape(slots, n, n_rep, height, width)),
        in_hbm(slot_grads),
        in_hbm(right_root),
    )
    rows = rows.reshape(n_rep * height, blocks, width)
    return pl.pallas_call(
        store,
        out_shape=(
            jax.ShapeDtypeStruct(sums.shape, sums.dtype),
            jax.ShapeDtypeStruct(rows.shape, rows.dtype),
        ),
        in_specs=[vmem_spec, vmem_spec],
        out_specs=(hbm_spec, hbm_spec),
        scratch_shapes=[dma((2,))],
    )(in_vmem(sums), in_vmem(rows))


def shards(tokens_x, key_grad, left_root, slot_grads, right_root, block_slot):
    n = lax.axis_size("shard")
    n_rep = lax.axis_size("rep")
    cols = tokens_x.shape[1] // n
    width = left_root.shape[2]
    per = left_root.shape[0] * left_root.shape[1] // (GROUP * n_rep)
    aligned = (
        n_rep == 2
        and n == 4 * GROUP
        and tokens_x.shape[1] % (n * PARTS * 128) == 0
        and key_grad.shape[1] % (n_rep * 128) == 0
        and 2 * key_grad.shape[1] == GROUP * PARTS * cols
        and tokens_x.shape[0] % 16 == 0
        and left_root.shape[1] % (n * n_rep * 16) == 0
        and width % (PIECES * 128) == 0
        and per % 128 == 0
        and block_slot.shape[0] % 16 == 0
        and left_root.shape[0] > 1
    )
    program = fused_shards if aligned else plain_shards
    return program(tokens_x, key_grad, left_root, slot_grads, right_root, block_slot)


def solution(mesh):
    return jax.shard_map(
        shards,
        mesh=mesh,
        in_specs=(
            P(("rep", "shard"), None),
            P(("rep", "shard"), None),
            P("shard", None, None),
            P("shard", None, None),
            P("shard", None, None),
            P(),
        ),
        out_specs=(P("shard", None), P("shard", None, None)),
        check_vma=False,
    )
```

```python
import jax
import jax.numpy as jnp
from jax import lax
from jax.experimental import pallas as pl
from jax.experimental.pallas import tpu as pltpu
from jax.sharding import PartitionSpec as P

MESH = pl.DeviceIdType.MESH
GROUP = 4
PARTS = 2
PIECES = 4
HALVES = 2


def column_term(features, cotangent):
    return lax.dot_general(
        features, cotangent, (((0,), (0,)), ((), ())), preferred_element_type=jnp.float32
    )


def precondition(left_block, grad_block, right_block):
    left_part = jnp.einsum(
        "sij,sjk->sik", left_block, grad_block, preferred_element_type=jnp.float32
    ).astype(jnp.bfloat16)
    return jnp.einsum(
        "sij,sjk->isk", left_part, right_block, preferred_element_type=jnp.float32
    ).astype(jnp.bfloat16)


def plain_shards(tokens_x, key_grad, left_root, slot_grads, right_root, block_slot):
    n_shard = lax.axis_size("shard")
    n_rep = lax.axis_size("rep")
    own_rows = lax.psum_scatter(
        column_term(tokens_x, key_grad), "shard", scatter_dimension=0, tiled=True
    )
    grad_key = lax.psum(own_rows, "rep")
    slot_count = left_root.shape[0]
    half_slots = slot_count // n_rep
    first_slot = lax.axis_index("rep") * half_slots

    def own_half(values):
        return lax.dynamic_slice_in_dim(values, first_slot, half_slots, 0)

    product = precondition(own_half(left_root), own_half(slot_grads), own_half(right_root))
    received = lax.all_to_all(product, "shard", split_axis=0, concat_axis=1, tiled=True)
    joined = lax.all_gather(received, "rep", axis=1, tiled=True)
    owner = block_slot // slot_count
    within = block_slot % slot_count
    position = (
        within // half_slots * (n_shard * half_slots) + owner * half_slots + within % half_slots
    )
    update = jnp.take(joined, position, axis=1)
    return (grad_key, update)


def remote(src, dst, send_sem, recv_sem, target):
    return pltpu.make_async_remote_copy(
        src_ref=src,
        dst_ref=dst,
        send_sem=send_sem,
        recv_sem=recv_sem,
        device_id=target,
        device_id_type=MESH,
    )


def kernel(
    where_ref, x_ref, g_ref, lr_ref, sg_ref, rr_ref, wide, rows,
    x_all, g_all, lr, sg, rr, prod, relay, upd, hot, part, met, kept, passed, first, second,
    x_own, part_own, met_own, kept_own, turned, got,
    sums, slot_ref,
    open_sem, load_sem, slot_load, x_load, send_sem, g_recv, x_recv, u_recv, y_recv, a_recv, s_recv, t_recv,
    r_recv, v_recv, d_load, d_recv, e_recv, f_recv,
):
    me = lax.axis_index("shard")
    rep = lax.axis_index("rep")
    other_rep = 1 - rep
    q = me % GROUP
    z = me // GROUP
    base = z * GROUP
    core = q + 1 - 2 * (q % 2)
    far = (q + 2) % GROUP
    both = (core + 2) % GROUP
    relatives = (q, core, far, both)
    z_near = z + 1 - 2 * (z % 2)
    z_half = (z + 2) % 4
    z_last = 3 - z
    order_of = (z_last, z_half, z_near, z)
    tok = g_ref.shape[0]
    unit = met.shape[1]
    half = met.shape[2]
    slots = lr.shape[0]
    n = lr.shape[1]
    height = lr.shape[2]
    width = lr.shape[3]
    blocks = slot_ref.shape[0]
    piece = width // PIECES

    def shard(index):
        return {"shard": index}

    across = {"rep": other_rep}
    near = shard(z_near * GROUP + q)
    opposite = shard(z_half * GROUP + q)

    def tokens_of(index):
        return pl.ds(index * tok, tok)

    def keys_of(side):
        return pl.ds(pl.multiple_of(side * half, 128), half)

    def columns(o, index, r):
        start = (order_of[o] * GROUP + index) * (PARTS * unit) + r * unit
        return pl.ds(pl.multiple_of(start, 128), unit)

    def unit_of(r):
        return pl.ds(r * unit, unit)

    copies_slot = []
    for s in range(slots):
        copies_slot.append(
            (
                pltpu.make_async_copy(lr_ref.at[s, :, rep], lr.at[s], slot_load.at[s, 0]),
                pltpu.make_async_copy(sg_ref.at[s], sg.at[s], slot_load.at[s, 1]),
                pltpu.make_async_copy(rr_ref.at[s], rr.at[s], slot_load.at[s, 2]),
            )
        )
    copy_g = pltpu.make_async_copy(g_ref, g_all.at[tokens_of(q)], load_sem.at[0])
    copies_x = []
    for o in range(3):
        start = pl.multiple_of((order_of[o] * GROUP + q) * (PARTS * unit), 128)
        copies_x.append(
            pltpu.make_async_copy(
                x_ref.at[:, pl.ds(start, PARTS * unit)], x_all.at[o, tokens_of(q)], x_load.at[o]
            )
        )

    lower = q - q % 2

    def wide_columns(index):
        start = (z * GROUP + index) * (PARTS * unit)
        return pl.ds(pl.multiple_of(start, 128), PARTS * unit)

    own_tokens = pl.ds((q % 2) * tok, tok)
    copies_own = []
    for w, index in enumerate((q, far)):
        copies_own.append(
            pltpu.make_async_copy(
                x_ref.at[:, wide_columns(index)], x_own.at[w, own_tokens], d_load.at[w]
            )
        )

    copy_g.start()
    barrier = pltpu.get_barrier_semaphore()
    peers = [across, near]
    for index in (core, far, both):
        peers.append(shard(base + index))
    inner = jnp.logical_and(z > 0, z < 3)
    facing = shard(z_last * GROUP + q)
    for peer in peers:
        pl.semaphore_signal(barrier, inc=1, device_id=peer, device_id_type=MESH)

    @pl.when(inner)
    def _():
        pl.semaphore_signal(barrier, inc=1, device_id=facing, device_id_type=MESH)

    copy_slot = pltpu.make_async_copy(where_ref, slot_ref, load_sem.at[1])
    copy_g.wait()
    for copy in copies_slot[0]:
        copy.start()
    for copy in copies_own:
        copy.start()
    for group in copies_slot[1:]:
        for copy in group:
            copy.start()
    for copy in copies_x:
        copy.start()
    copy_slot.start()
    @pl.when(inner)
    def _():
        pl.semaphore_wait(barrier, len(peers) + 1)
        pl.semaphore_signal(open_sem, inc=1, device_id=facing, device_id_type=MESH)

    @pl.when(jnp.logical_not(inner))
    def _():
        pl.semaphore_wait(barrier, len(peers))


    def send(src, dst, kind, recv_sem, target):
        remote(src, dst, send_sem.at[kind], recv_sem, target).start()

    def arrive(ref, recv_sem):
        remote(ref, ref, send_sem.at[0], recv_sem, across).wait_recv()

    def send_g(which, target, place):
        keys = keys_of(other_rep if which == 0 else rep)
        view = g_all.at[tokens_of(q), keys]
        send(view, view, 0, g_recv.at[which, place], shard(base + target))

    def send_x(o, r):
        for target in (far, both, core):
            send(
                x_ref.at[:, columns(o, target, r)],
                x_all.at[o, tokens_of(q), unit_of(r)],
                1,
                x_recv.at[o, r],
                shard(base + target),
            )

    send_g(0, far, 0)
    for r in range(PARTS):
        send_x(0, r)
    send_g(0, core, 1)
    for w, index in enumerate((core, both)):
        send(
            x_ref.at[:, wide_columns(index)], x_own.at[w, own_tokens], 9, d_recv.at[w],
            shard(base + core),
        )
    send_g(1, core, 1)
    send_g(1, far, 0)
    for o in (1, 2):
        for r in range(PARTS):
            send_x(o, r)

    pair = pl.ds(lower * tok, 2 * tok)
    mate_tokens = pl.ds((1 - q % 2) * tok, tok)

    def partial_own(w, r, side):
        return lax.dot_general(
            x_own[w, :, r * unit : (r + 1) * unit],
            g_all[pair, keys_of(side)],
            (((0,), (0,)), ((), ())),
            preferred_element_type=jnp.float32,
        )

    def give_own(w, r):
        v = w * PARTS + r
        part_own[v] = partial_own(w, r, other_rep).astype(jnp.bfloat16)
        send(part_own.at[v], met_own.at[v], 10, e_recv.at[v], across)

    def keep_own(w, r):
        kept_own[w * PARTS + r] = partial_own(w, r, rep)

    def total_own(w, r):
        v = w * PARTS + r
        arrive(met_own.at[v], e_recv.at[v])
        return kept_own[v] + met_own[v].astype(jnp.float32)

    def turn(r):
        turned[r] = total_own(1, r).astype(jnp.bfloat16)

    def send_turned(r):
        send(turned.at[r], got.at[r], 11, f_recv.at[r], shard(base + far))

    def send_slot(s, levels):
        for level in levels:
            send(prod.at[level, s], relay.at[z, s], 2, u_recv.at[0], shard(level * GROUP + q))

    for s in range(slots):
        for copy in copies_slot[s]:
            copy.wait()
        left = jnp.dot(
            lr[s].reshape(n * height, width), sg[s], preferred_element_type=jnp.float32
        ).astype(jnp.bfloat16)
        full = jnp.dot(left, rr[s], preferred_element_type=jnp.float32).astype(jnp.bfloat16)
        prod[:, s] = full.reshape(4, GROUP, height, width)
        if s == 0:

            @pl.when(inner)
            def _():
                pl.semaphore_wait(open_sem, 1)
                pl.semaphore_signal(open_sem, inc=1, device_id=near, device_id_type=MESH)

            send_slot(s, (z_near,))
        elif s == 1:

            @pl.when(jnp.logical_not(inner))
            def _():
                pl.semaphore_wait(open_sem, 1)

            send_slot(0, (z_last, z_half))
            send_slot(1, (z_last, z_half, z_near))
        else:
            send_slot(s, (z_last, z_half, z_near))

    arrive(g_all.at[tokens_of(core), keys_of(other_rep)], g_recv.at[0, 1])
    for w in range(2):
        copies_own[w].wait()
        arrive(x_own.at[w, mate_tokens], d_recv.at[w])
    for r in range(PARTS):
        give_own(1, r)

    copy_slot.wait()
    chosen = jnp.zeros((blocks, 128), jnp.int32)
    row = lax.broadcasted_iota(jnp.int32, (blocks, 128), 0)
    for b in range(blocks):
        chosen = jnp.where(row == b, slot_ref[b], chosen)
    lane = lax.broadcasted_iota(jnp.int32, (blocks, 128), 1)
    per = 4 * slots * height
    for k, index in enumerate(relatives):
        for part_of in range(per // 128):
            place = lane + part_of * 128
            source = place // (slots * height) * (GROUP * slots) + index * slots
            source = source + place // height % slots
            same = source == chosen
            for i in range(height):
                hit = jnp.logical_and(same, place % height == i)
                hot[k, pl.ds(i * blocks, blocks), pl.ds(part_of * 128, 128)] = jnp.where(
                    hit, 1.0, 0.0
                ).astype(jnp.bfloat16)

    relay[z] = prod[z]

    def gather_g(which):
        keys = keys_of(other_rep if which == 0 else rep)
        view = g_all.at[tokens_of(far), keys]
        arrive(view, g_recv.at[which, 0])
        send(view, view, 0, g_recv.at[which, 2], shard(base + core))
        arrive(g_all.at[tokens_of(both), keys], g_recv.at[which, 2])

    def partial(o, r, side):
        return lax.dot_general(
            x_all[o, :, r * unit : (r + 1) * unit],
            g_all[:, keys_of(side)],
            (((0,), (0,)), ((), ())),
            preferred_element_type=jnp.float32,
        )

    def give(o, r):
        if r == 0:
            copies_x[o].wait()
        arrive(x_all.at[o, pl.ds(0, 3 * tok), unit_of(r)], x_recv.at[o, r])
        part[o * PARTS + r] = partial(o, r, other_rep).astype(jnp.bfloat16)
        send(
            part.at[o * PARTS + r], met.at[o * PARTS + r], 3, a_recv.at[o * PARTS + r], across
        )

    def keep(o, r):
        kept[o * PARTS + r] = partial(o, r, rep)

    def total_of(o, r):
        u = o * PARTS + r
        arrive(met.at[u], a_recv.at[u])
        return kept[u] + met[u].astype(jnp.float32)

    def pass_near(o, r):
        u = o // 2 * PARTS + r
        passed[u] = total_of(o, r).astype(jnp.bfloat16)
        send(passed.at[u], first.at[u], 4, s_recv.at[u], near)

    def pass_half(r):
        u = 2 * PARTS + r
        total = total_of(1, r)
        arrive(first.at[r], s_recv.at[r])
        passed[u] = (total + first[r].astype(jnp.float32)).astype(jnp.bfloat16)
        send(passed.at[u], second.at[r], 5, t_recv.at[r], opposite)

    def finish(r):
        total = total_own(0, r)
        arrive(got.at[r], f_recv.at[r])
        total = total + got[r].astype(jnp.float32)
        arrive(second.at[r], t_recv.at[r])
        total = total + second[r].astype(jnp.float32)
        arrive(first.at[PARTS + r], s_recv.at[PARTS + r])
        total = total + first[PARTS + r].astype(jnp.float32)
        view = sums.at[rep, unit_of(r)]
        sums[rep, unit_of(r)] = total.astype(jnp.bfloat16)
        send(view, view, 6, r_recv.at[r], across)

    def slice_of(p):
        return pl.ds(p * piece, piece)

    def spread(p):
        for k, target in ((2, far), (3, both), (1, core)):
            send(
                relay.at[:, :, target, :, slice_of(p)],
                upd.at[k, :, :, :, slice_of(p)],
                7,
                y_recv.at[k // 2, p],
                shard(base + target),
            )

    lines = height // HALVES

    def select(p):
        cols = slice(p * piece, (p + 1) * piece)

        def block(k):
            return upd[k, :, :, :, cols].reshape(per, piece)

        arrive(upd.at[1, :, :, :, slice_of(p)], y_recv.at[0, p])
        early = jnp.dot(
            hot[0], relay[:, :, q, :, cols].reshape(per, piece), preferred_element_type=jnp.float32
        ) + jnp.dot(hot[1], block(1), preferred_element_type=jnp.float32)
        arrive(upd.at[pl.ds(2, 2), :, :, :, slice_of(p)], y_recv.at[1, p])
        for h in range(HALVES):
            here = slice(h * lines * blocks, (h + 1) * lines * blocks)
            value = early[here]
            for k in (2, 3):
                value = value + jnp.dot(
                    hot[k, here], block(k), preferred_element_type=jnp.float32
                )
            rows[rep, h * lines : (h + 1) * lines, :, cols] = value.astype(jnp.bfloat16).reshape(
                lines, blocks, piece
            )
            view = rows.at[rep, pl.ds(h * lines, lines), :, slice_of(p)]
            send(view, view, 8, v_recv.at[p, h], across)

    def widen(side, r):
        wide[unit_of(r), keys_of(side)] = sums[side, unit_of(r)].astype(jnp.float32)

    arrive(g_all.at[tokens_of(core), keys_of(rep)], g_recv.at[1, 1])
    for w in (1, 0):
        for r in range(PARTS):
            keep_own(w, r)
    gather_g(0)
    give(0, 0)
    give(0, 1)
    for r in range(PARTS):
        give_own(0, r)
    gather_g(1)
    keep(0, 0)
    keep(0, 1)
    pass_near(0, 0)
    give(1, 0)
    keep(1, 0)
    pass_near(0, 1)
    give(1, 1)
    keep(1, 1)
    turn(0)
    turn(1)
    give(2, 0)
    keep(2, 0)
    arrive(relay.at[pl.ds(0, 3)], u_recv.at[0])
    spread(0)
    spread(1)
    spread(2)
    send_turned(0)
    spread(3)
    send_turned(1)
    pass_half(0)
    give(2, 1)
    keep(2, 1)
    pass_half(1)
    pass_near(2, 0)
    select(0)
    pass_near(2, 1)
    select(1)
    select(2)
    finish(0)
    select(3)
    finish(1)
    widen(rep, 0)
    widen(rep, 1)
    for r in range(PARTS):
        arrive(sums.at[other_rep, unit_of(r)], r_recv.at[r])
        widen(other_rep, r)
    for p in range(PIECES):
        for h in range(HALVES):
            arrive(
                rows.at[other_rep, pl.ds(h * lines, lines), :, slice_of(p)], v_recv.at[p, h]
            )

    def drain(ref, kind):
        remote(ref, ref, send_sem.at[kind], send_sem.at[kind], across).wait_send()

    drain(x_all, 0)
    drain(x_all.at[:, pl.ds(0, 3 * tok)], 1)
    drain(relay.at[pl.ds(0, 3)], 2)
    drain(met, 3)
    drain(prod.at[0], 9)
    drain(met_own, 10)
    drain(got, 11)
    drain(met.at[pl.ds(0, 2 * PARTS)], 4)
    drain(met.at[pl.ds(0, PARTS)], 5)
    drain(met.at[pl.ds(0, PARTS)], 6)
    drain(relay.at[pl.ds(0, 3)], 7)
    drain(rows.at[0], 8)


def in_hbm(array):
    return pltpu.with_memory_space_constraint(array, pltpu.HBM)


def in_vmem(array):
    return pltpu.with_memory_space_constraint(array, pltpu.VMEM)


def store(sums_ref, rows_ref, og_ref, ou_ref, sem):
    copies = (
        pltpu.make_async_copy(sums_ref, og_ref, sem.at[0]),
        pltpu.make_async_copy(rows_ref, ou_ref, sem.at[1]),
    )
    for copy in copies:
        copy.start()
    for copy in copies:
        copy.wait()


def fused_shards(tokens_x, key_grad, left_root, slot_grads, right_root, block_slot):
    n = lax.axis_size("shard")
    n_rep = lax.axis_size("rep")
    tok, d_model = tokens_x.shape
    key_width = key_grad.shape[1]
    cols = d_model // n
    slots, order_b, width = left_root.shape
    height = order_b // n // n_rep
    blocks = block_slot.shape[0]
    half = key_width // n_rep
    unit = cols // PARTS
    per = 4 * slots * height
    bf16, f32 = jnp.bfloat16, jnp.float32
    dma = pltpu.SemaphoreType.DMA
    hbm_spec = pl.BlockSpec(memory_space=pltpu.HBM)
    vmem_spec = pl.BlockSpec(memory_space=pltpu.VMEM)
    sums, rows = pl.pallas_call(
        kernel,
        out_shape=(
            pltpu.VMEM((cols, key_width), f32),
            pltpu.VMEM((n_rep, height, blocks, width), bf16),
        ),
        in_specs=[hbm_spec] * 6,
        out_specs=(vmem_spec, vmem_spec),
        scratch_shapes=[
            pltpu.VMEM((3, GROUP * tok, cols), bf16),
            pltpu.VMEM((GROUP * tok, key_width), bf16),
            pltpu.VMEM((slots, n, height, width), bf16),
            pltpu.VMEM(slot_grads.shape, bf16),
            pltpu.VMEM(right_root.shape, bf16),
            pltpu.VMEM((4, slots, GROUP, height, width), bf16),
            pltpu.VMEM((4, slots, GROUP, height, width), bf16),
            pltpu.VMEM((4, 4, slots, height, width), bf16),
            pltpu.VMEM((4, height * blocks, per), bf16),
            pltpu.VMEM((3 * PARTS, unit, half), bf16),
            pltpu.VMEM((3 * PARTS, unit, half), bf16),
            pltpu.VMEM((3 * PARTS, unit, half), f32),
            pltpu.VMEM((3 * PARTS, unit, half), bf16),
            pltpu.VMEM((2 * PARTS, unit, half), bf16),
            pltpu.VMEM((PARTS, unit, half), bf16),
            pltpu.VMEM((2, 2 * tok, cols), bf16),
            pltpu.VMEM((2 * PARTS, unit, half), bf16),
            pltpu.VMEM((2 * PARTS, unit, half), bf16),
            pltpu.VMEM((2 * PARTS, unit, half), f32),
            pltpu.VMEM((PARTS, unit, half), bf16),
            pltpu.VMEM((PARTS, unit, half), bf16),
            pltpu.VMEM((n_rep, cols, half), bf16),
            pltpu.SMEM(block_slot.shape, jnp.int32),
            pltpu.SemaphoreType.REGULAR,
            dma((2,)),
            dma((slots, 3)),
            dma((3,)),
            dma((12,)),
            dma((2, 3)),
            dma((3, PARTS)),
            dma((1,)),
            dma((2, PIECES)),
            dma((3 * PARTS,)),
            dma((2 * PARTS,)),
            dma((PARTS,)),
            dma((PARTS,)),
            dma((PIECES, HALVES)),
            dma((2,)),
            dma((2,)),
            dma((2 * PARTS,)),
            dma((PARTS,)),
        ],
        compiler_params=pltpu.CompilerParams(
            collective_id=0, has_side_effects=True, vmem_limit_bytes=48 * 1024 * 1024
        ),
    )(
        in_hbm(block_slot),
        in_hbm(tokens_x),
        in_hbm(key_grad),
        in_hbm(left_root.reshape(slots, n, n_rep, height, width)),
        in_hbm(slot_grads),
        in_hbm(right_root),
    )
    rows = rows.reshape(n_rep * height, blocks, width)
    return pl.pallas_call(
        store,
        out_shape=(
            jax.ShapeDtypeStruct(sums.shape, sums.dtype),
            jax.ShapeDtypeStruct(rows.shape, rows.dtype),
        ),
        in_specs=[vmem_spec, vmem_spec],
        out_specs=(hbm_spec, hbm_spec),
        scratch_shapes=[dma((2,))],
    )(in_vmem(sums), in_vmem(rows))


def shards(tokens_x, key_grad, left_root, slot_grads, right_root, block_slot):
    n = lax.axis_size("shard")
    n_rep = lax.axis_size("rep")
    cols = tokens_x.shape[1] // n
    width = left_root.shape[2]
    per = left_root.shape[0] * left_root.shape[1] // (GROUP * n_rep)
    aligned = (
        n_rep == 2
        and n == 4 * GROUP
        and tokens_x.shape[1] % (n * PARTS * 128) == 0
        and key_grad.shape[1] % (n_rep * 128) == 0
        and 2 * key_grad.shape[1] == GROUP * PARTS * cols
        and tokens_x.shape[0] % 16 == 0
        and left_root.shape[1] % (n * n_rep * 16) == 0
        and width % (PIECES * 128) == 0
        and per % 128 == 0
        and block_slot.shape[0] % 16 == 0
        and left_root.shape[0] > 1
    )
    program = fused_shards if aligned else plain_shards
    return program(tokens_x, key_grad, left_root, slot_grads, right_root, block_slot)


def solution(mesh):
    return jax.shard_map(
        shards,
        mesh=mesh,
        in_specs=(
            P(("rep", "shard"), None),
            P(("rep", "shard"), None),
            P("shard", None, None),
            P("shard", None, None),
            P("shard", None, None),
            P(),
        ),
        out_specs=(P("shard", None), P("shard", None, None)),
        check_vma=False,
    )
```
